256 devices in a mesh: grp: 4 (over x), row: 64 (over y, z, core).
Axes of the slice: x: 4, y: 4, z: 8, core: 2. Of those that a mesh axis runs over, the one named last changes fastest.
Arguments:
- snapshots: float32 [229376, 2048], P('row', 'grp'), may hold values from -24 to 24, as said below
- test_block: float32 [229376, 512], P('row', 'grp'), may hold values from -24 to 24, as said below
- start_block: float32 [2048, 64], P('grp'), may hold values from -6 to 6
- start_merge: float32 [256, 64], replicated, may hold values from -6 to 6
Outputs:
- projected: float32 [229376, 512], P('row', 'grp')
The draws below stay inside these ranges and needn't reach their ends.
Inputs may be any that keep to these rules, and one draw needn't show every extreme that they name: snapshots are float32 values of order one, full rank. test_block holds float32 values of order one.
All inputs are finite; a program needn't handle non-finite values.
Results may differ from the reference program's by a relative error of at most 0.0003.
Values sent between devices are 32-bit elements; how exact they have to be, the bound alone decides.
No kernel may reach another device: no remote copies, remote signals or barrier semaphores. Data moves between devices by JAX's collectives and lax.ppermute only.
A program may use at most 64 MiB of HBM per device.

```python
import math
import jax
import jax.numpy as jnp
from jax import lax

SNAP_G = 512
RANK = 64
ITERS = 6
NROWS = 229376
SNAP = 2048
TEST = 512
WIDE = 256
N_GRP = 4


def shared_fields(key):
    base_key = jax.random.fold_in(key, 101)
    key_factor, key_scale, key_strength = jax.random.split(base_key, 3)
    factors = jnp.clip(jax.random.normal(key_factor, (NROWS, 96), jnp.float32), -4.0, 4.0)
    row_scale = jnp.exp(jax.random.uniform(key_scale, (NROWS, 1), jnp.float32, -0.5, 0.5))
    strength = jnp.exp(jax.random.uniform(key_strength, (96, 1), jnp.float32, math.log(0.3), math.log(3.0)))
    return (factors, row_scale, strength)


def build_field(key, salt, columns, weight, noise_low, noise_high):
    factors, row_scale, strength = shared_fields(key)
    own_key = jax.random.fold_in(key, salt)
    key_mix, key_noise, key_column = jax.random.split(own_key, 3)
    mixing = jnp.clip(jax.random.normal(key_mix, (96, columns), jnp.float32), -4.0, 4.0) * strength * weight
    column_scale = jnp.exp(jax.random.uniform(key_column, (1, columns), jnp.float32, math.log(noise_low), math.log(noise_high)))
    noise_part = jnp.clip(jax.random.normal(key_noise, (NROWS, columns), jnp.float32), -4.0, 4.0) * column_scale
    field = jnp.dot(factors, mixing, precision=lax.Precision.HIGHEST) + noise_part
    return jnp.clip(row_scale * field, -24.0, 24.0).astype(jnp.float32)


def draw_snapshots(key, part):
    return build_field(key, 202, SNAP, 1.0 / math.sqrt(SNAP_G), 0.3, 2.0)


def draw_test_block(key, part):
    return build_field(key, 303, TEST, 0.1, 0.3, 1.0)


def level_of(stream_key, shape, shards, low, largest):
    def one(dim, shards_of):
        steps = jax.random.uniform(jax.random.fold_in(jax.random.fold_in(stream_key, 6), dim), (shards_of,), jnp.float32, low / len(shards), largest / len(shards))
        return jnp.repeat(jnp.exp(steps), shape[dim] // shards_of).reshape((-1,) + (1,) * (len(shape) - dim - 1))

    loudness = one(*shards[0])
    for cut in shards[1:]:
        loudness = loudness * one(*cut)
    return loudness


def centred(key, extent, width, bound, cuts=(), held_as=jnp.bfloat16):
    array = jax.random.normal(key, extent, jnp.float32) * width
    if len(cuts) > 0:
        array = level_of(key, extent, cuts, -0.22, 0.18) * array
    return jnp.clip(array, min=-bound, max=bound).astype(held_as)


def setup_inputs(seed: int = 0) -> dict:
    key_list = jax.random.split(jax.random.key(seed), 5)
    snapshots = draw_snapshots(jax.random.fold_in(key_list[4], 71), 0)
    test_block = draw_test_block(jax.random.fold_in(key_list[4], 71), 0)
    start_block = centred(key_list[2], (SNAP, RANK), 1.0, 6.0, ((0, 4),), jnp.float32)
    start_merge = centred(key_list[3], (WIDE, RANK), 1.0, 6.0, (), jnp.float32)
    return dict(snapshots=snapshots, test_block=test_block, start_block=start_block, start_merge=start_merge)


def highdot(left, right):
    return jnp.dot(left.astype(jnp.float32), right.astype(jnp.float32), precision=lax.Precision.HIGHEST, preferred_element_type=jnp.float32)

def orthonormal(tall_block):
    small_gram = highdot(tall_block.T, tall_block)
    lower_factor = jnp.linalg.cholesky(small_gram)
    return lax.linalg.triangular_solve(lower_factor, tall_block, left_side=False, lower=True, transpose_a=True)

def reference(snapshots, test_block, start_block, start_merge):
    row_total = snapshots.shape[0]
    group_bases = []
    for group_index in range(N_GRP):
        columns = snapshots[:, group_index * SNAP_G:(group_index + 1) * SNAP_G]
        full_gram = highdot(columns.T, columns) / row_total
        iterate = orthonormal(start_block[group_index * SNAP_G:(group_index + 1) * SNAP_G])
        for sweep_index in range(ITERS):
            iterate = orthonormal(highdot(full_gram, iterate))
        group_bases.append(highdot(columns, iterate))
    joined = jnp.concatenate(group_bases, axis=1)
    merged_gram = highdot(joined.T, joined) / row_total
    merge_coef = orthonormal(start_merge)
    for sweep_index in range(ITERS):
        merge_coef = orthonormal(highdot(merged_gram, merge_coef))
    energy = highdot(merge_coef.T, highdot(merged_gram, merge_coef))
    lower_factor = jnp.linalg.cholesky(energy)
    merge_coef = lax.linalg.triangular_solve(lower_factor, merge_coef, left_side=False, lower=True, transpose_a=True)
    merged_modes = highdot(joined, merge_coef) / math.sqrt(row_total)
    return highdot(merged_modes, highdot(merged_modes.T, test_block))
```

```python
import jax
import jax.numpy as jnp
from jax import lax
from jax.experimental import pallas as pl
from jax.experimental.pallas import tpu as pltpu
from jax.sharding import Mesh
from jax.sharding import PartitionSpec as P

ITERS = 6
ROW = ("row_0", "row_1", "row_2")
CHIPS = ("row_0", "row_1")
CORE = "row_2"
BLOCK = 128
VMEM = pl.BlockSpec(memory_space=pltpu.VMEM)
SMEM = pl.BlockSpec(memory_space=pltpu.SMEM)

NT = (((1,), (1,)), ((), ()))
NN = (((1,), (0,)), ((), ()))
TN = (((0,), (0,)), ((), ()))


def dot(left, right, dims):
    return lax.dot_general(left, right, dims, preferred_element_type=jnp.float32)


def parts(x, count):
    found = []
    for _ in range(count - 1):
        piece = x.astype(jnp.bfloat16)
        found.append(piece)
        x = x - piece.astype(jnp.float32)
    found.append(x.astype(jnp.bfloat16))
    return found


def dot_parts(left, right, dims):
    count = len(left)
    rows = left[0].shape[0]
    total = None
    for j in reversed(range(count)):
        stack = jnp.concatenate(left[: count - j], axis=0) if j < count - 1 else left[0]
        product = dot(stack, right[j], dims)
        for i in reversed(range(count - j)):
            piece = product[i * rows : (i + 1) * rows]
            total = piece if total is None else total + piece
    return total


def lower_inverse(matrix):
    size = matrix.shape[0]
    bands = size // 8
    sub = lax.broadcasted_iota(jnp.int32, (8, 2 * size), 0)
    lane = lax.broadcasted_iota(jnp.int32, (8, 2 * size), 1)
    wide = jnp.concatenate([matrix, jnp.zeros_like(matrix)], axis=1)
    work = [
        jnp.where(lane == size + 8 * b + sub, 1.0, wide[8 * b : 8 * b + 8]) for b in range(bands)
    ]

    def column(value, j):
        return jnp.broadcast_to(value[:, j : j + 1], value.shape)

    def line(value, j):
        return jnp.broadcast_to(value[j : j + 1, :], value.shape)

    for b in range(bands):
        cols = {i: [column(work[i], 8 * b + j) for j in range(8)] for i in range(b, bands)}
        scale = None
        for j in range(8):
            pivot = line(cols[b][j], j)
            inverse = 1.0 / pivot
            root = lax.rsqrt(pivot)
            scale = root if scale is None else jnp.where(sub == j, root, scale)
            factor = jnp.where(sub > j, cols[b][j] * inverse, 0.0)
            ahead = {k: line(cols[b][k], j) for k in range(j + 1, 8)}
            pivot_row = line(work[b], j)
            for k in range(j + 1, 8):
                cols[b][k] = cols[b][k] - factor * ahead[k]
            work[b] = work[b] - factor * pivot_row
            for i in range(b + 1, bands):
                below = cols[i][j] * inverse
                for k in range(j + 1, 8):
                    cols[i][k] = cols[i][k] - below * ahead[k]
                work[i] = work[i] - below * pivot_row
        work[b] = work[b] * scale
    return jnp.concatenate(work, axis=0)[:, size:]


def orthonormal(rows):
    split = parts(rows, 3)
    return dot_parts(parts(lower_inverse(dot_parts(split, split, NT)), 3), split, NN)


def upper_pairs(count):
    return [(a, b) for a in range(count) for b in range(a, count)]


def cut(index):
    return slice(index * BLOCK, (index + 1) * BLOCK)


def gram_kernel(core_ref, x_ref, o_ref, held_ref, arrived, *sum_refs):
    steps, deep, width = held_ref.shape
    half = width // 2
    copies = [
        pltpu.make_async_copy(
            x_ref.at[pl.ds(n * deep, deep), :], held_ref.at[n], arrived.at[n]
        )
        for n in range(steps)
    ]
    for copy in copies:
        copy.start()
    left, right = slice(None, half), slice(half, None)
    for n, copy in enumerate(copies):
        copy.wait()
        high, low = parts(held_ref[n], 2)
        high_t, low_t = high.T, low.T
        found = [
            dot(high_t[left], high[:, left], NN) + dot(low_t[left], low[:, left], NN),
            dot(high_t[left], high[:, right], NN) + dot(low_t[left], low[:, right], NN),
            dot(high_t[right], high[:, right], NN) + dot(low_t[right], low[:, right], NN),
            dot(high_t[left], low[:, left], NN),
            dot(high_t[left], low[:, right], NN),
            dot(high_t[right], low[:, left], NN),
            dot(high_t[right], low[:, right], NN),
        ]
        for ref, value in zip(sum_refs, found):
            ref[...] = value if n == 0 else ref[...] + value
    aa, ab, bb, ll, lr, rl, rr = [ref[...] for ref in sum_refs]
    place = {(0, 0): aa + ll + ll.T, (0, 1): ab + lr + rl.T, (1, 1): bb + rr + rr.T}
    pairs = upper_pairs(width // BLOCK)
    held = len(pairs) // 2
    for n, (a, b) in enumerate(pairs):
        block = place[a // 2, b // 2][cut(a % 2), cut(b % 2)]
        o_ref[(n // held) ^ core_ref[0], cut(n % held), :] = block


def gram(snapshots, core):
    rows, width = snapshots.shape
    steps = 4
    held = len(upper_pairs(width // BLOCK)) // 2 * BLOCK
    return pl.pallas_call(
        gram_kernel,
        in_specs=[SMEM, pl.BlockSpec(memory_space=pl.ANY)],
        out_specs=VMEM,
        out_shape=jax.ShapeDtypeStruct((2, held, BLOCK), jnp.float32),
        scratch_shapes=[
            pltpu.VMEM((steps, rows // steps, width), jnp.float32),
            pltpu.SemaphoreType.DMA((steps,)),
        ]
        + [pltpu.VMEM((width // 2, width // 2), jnp.float32)] * 7,
        compiler_params=pltpu.CompilerParams(vmem_limit_bytes=48 * 2**20),
        name="gram",
    )(core, snapshots)


def in_order(core_ref, mine_ref, other_ref):
    first = core_ref[0] == 0
    mine, other = mine_ref[...], other_ref[...]
    return jnp.where(first, mine, other), jnp.where(first, other, mine)


def sweep(basis_ref, next_ref, gram_refs, last):
    basis = orthonormal(next_ref[...])
    basis_ref[...] = basis

    @pl.when(jnp.logical_not(last))
    def _():
        next_ref[...] = dot_parts(parts(basis, 3), [r[...] for r in gram_refs], NN)


def solve_kernel(row_total, core_ref, mine_ref, other_ref, start_ref, o_ref, next_ref, *gram_refs):
    width = gram_refs[0].shape[0]
    pairs = upper_pairs(width // BLOCK)
    held = len(pairs) // 2
    halves = in_order(core_ref, mine_ref, other_ref)
    for n, (a, b) in enumerate(pairs):
        block = halves[n // held][cut(n % held)] / row_total
        for ref, piece in zip(gram_refs, parts(block, 3)):
            ref[cut(a), cut(b)] = piece
        if a != b:
            for ref, piece in zip(gram_refs, parts(block.T, 3)):
                ref[cut(b), cut(a)] = piece
    next_ref[...] = start_ref[...].T

    def step(index, carry):
        sweep(o_ref, next_ref, gram_refs, index == ITERS)
        return carry

    lax.fori_loop(0, ITERS + 1, step, 0)


def group_solve(core, mine, other, start, row_total):
    width, rank = start.shape
    return pl.pallas_call(
        lambda *refs: solve_kernel(row_total, *refs),
        in_specs=[SMEM, VMEM, VMEM, VMEM],
        out_specs=VMEM,
        out_shape=jax.ShapeDtypeStruct((rank, width), jnp.float32),
        scratch_shapes=[pltpu.VMEM((rank, width), jnp.float32)]
        + [pltpu.VMEM((width, width), jnp.bfloat16)] * 3,
        compiler_params=pltpu.CompilerParams(vmem_limit_bytes=32 * 2**20),
        name="group_solve",
    )(core, mine, other, start)


def basis_kernel(q_ref, x_ref, o_ref):
    o_ref[...] = dot_parts(parts(q_ref[...], 2), parts(x_ref[...], 2), NT)


def group_basis(basis, snapshots):
    rank, width = basis.shape
    rows = snapshots.shape[0]
    step = rows // 4
    return pl.pallas_call(
        basis_kernel,
        grid=(rows // step,),
        in_specs=[
            pl.BlockSpec((rank, width), lambda i: (0, 0)),
            pl.BlockSpec((step, width), lambda i: (i, 0)),
        ],
        out_specs=pl.BlockSpec((rank, step), lambda i: (0, i)),
        out_shape=jax.ShapeDtypeStruct((rank, rows), jnp.float32),
        compiler_params=pltpu.CompilerParams(
            dimension_semantics=("arbitrary",), vmem_limit_bytes=48 * 2**20
        ),
        name="group_basis",
    )(basis, snapshots)


def merge_kernel(core_ref, joined_ref, test_ref, o_ref, gram_ref, side_ref):
    step = pl.program_id(0)

    @pl.when(step == 0)
    def _():
        gram_ref[...] = jnp.zeros_like(gram_ref)
        side_ref[...] = jnp.zeros_like(side_ref)

    left = parts(joined_ref[...], 2)
    gram_ref[...] += dot_parts(left, left, NT)
    side_ref[...] += dot_parts(left, parts(test_ref[...], 2), NN)

    @pl.when(step == pl.num_programs(0) - 1)
    def _():
        blocks = [gram_ref[cut(a), cut(b)] for a, b in upper_pairs(2)]
        blocks += [side_ref[cut(a), :] for a in range(2)]
        pieces = [block[i * 64 : (i + 1) * 64] for block in blocks for i in range(2)]
        for n, piece in enumerate(pieces):
            o_ref[(n // 5) ^ core_ref[0], (n % 5) * 64 : (n % 5 + 1) * 64, :] = piece


def merge_partials(core, joined, test_block):
    wide, rows = joined.shape
    step = rows // 4
    return pl.pallas_call(
        merge_kernel,
        grid=(rows // step,),
        in_specs=[
            SMEM,
            pl.BlockSpec((wide, step), lambda i: (0, i)),
            pl.BlockSpec((step, BLOCK), lambda i: (i, 0)),
        ],
        out_specs=pl.BlockSpec((2, 320, BLOCK), lambda i: (0, 0, 0)),
        out_shape=jax.ShapeDtypeStruct((2, 320, BLOCK), jnp.float32),
        scratch_shapes=[
            pltpu.VMEM((wide, wide), jnp.float32),
            pltpu.VMEM((wide, BLOCK), jnp.float32),
        ],
        compiler_params=pltpu.CompilerParams(
            dimension_semantics=("arbitrary",), vmem_limit_bytes=48 * 2**20
        ),
        name="merge_partials",
    )(core, joined, test_block)


def finish_kernel(
    row_total, core_ref, mine_ref, other_ref, start_ref, joined_ref, o_ref,
    next_ref, coef_ref, weight_ref, *gram_refs
):
    step_index = pl.program_id(0)

    @pl.when(step_index == 0)
    def _():
        halves = in_order(core_ref, mine_ref, other_ref)
        pieces = [halves[n // 5][(n % 5) * 64 : (n % 5 + 1) * 64] for n in range(10)]
        blocks = [jnp.concatenate(pieces[2 * n : 2 * n + 2], axis=0) for n in range(5)]
        for (a, b), block in zip(upper_pairs(2), blocks[:3]):
            block = block / row_total
            for ref, piece in zip(gram_refs, parts(block, 3)):
                ref[cut(a), cut(b)] = piece
            if a != b:
                for ref, piece in zip(gram_refs, parts(block.T, 3)):
                    ref[cut(b), cut(a)] = piece
        next_ref[...] = start_ref[...].T

        def step(index, carry):
            sweep(coef_ref, next_ref, gram_refs, index > ITERS)
            return carry

        lax.fori_loop(0, ITERS + 1, step, 0)
        coef = parts(coef_ref[...], 3)
        energy = dot_parts(parts(next_ref[...], 3), coef, NT)
        coef = dot_parts(parts(lower_inverse(energy), 3), coef, NN)
        coef_parts = parts(coef, 3)
        side = jnp.concatenate(blocks[3:], axis=0)
        test_coeffs = dot_parts(coef_parts, parts(side, 3), NN)
        weight_ref[...] = dot_parts(parts(coef.T, 3), parts(test_coeffs, 3), NN) / row_total

    o_ref[...] = dot_parts(parts(joined_ref[...].T, 2), parts(weight_ref[...], 2), NN)


def finish(core, mine, other, start, joined, row_total):
    wide, rows = joined.shape
    rank = start.shape[1]
    step = rows // 4
    return pl.pallas_call(
        lambda *refs: finish_kernel(row_total, *refs),
        grid=(rows // step,),
        in_specs=[SMEM, VMEM, VMEM, VMEM, pl.BlockSpec((wide, step), lambda i: (0, i))],
        out_specs=pl.BlockSpec((step, BLOCK), lambda i: (i, 0)),
        out_shape=jax.ShapeDtypeStruct((rows, BLOCK), jnp.float32),
        scratch_shapes=[
            pltpu.VMEM((rank, wide), jnp.float32),
            pltpu.VMEM((rank, wide), jnp.float32),
            pltpu.VMEM((wide, BLOCK), jnp.float32),
        ]
        + [pltpu.VMEM((wide, wide), jnp.bfloat16)] * 3,
        compiler_params=pltpu.CompilerParams(
            dimension_semantics=("arbitrary",), vmem_limit_bytes=48 * 2**20
        ),
        name="finish",
    )(core, mine, other, start, joined)


def swap_cores(array):
    return lax.ppermute(array, CORE, [(0, 1), (1, 0)])


def sum_over_rows(halves):
    kept = halves[0] + swap_cores(halves[1])
    chips = lax.axis_size(CHIPS)
    cuts = kept.reshape(chips, kept.shape[0] // chips, BLOCK)
    own = jnp.sum(lax.all_to_all(cuts, CHIPS, 0, 0, tiled=True), axis=0)
    copies = jnp.broadcast_to(own, (chips, *own.shape))
    mine = lax.all_to_all(copies, CHIPS, 0, 0, tiled=True).reshape(kept.shape)
    return mine, swap_cores(mine)


def on_device(snapshots, test_block, start_block, start_merge):
    row_total = snapshots.shape[0] * lax.axis_size(ROW)
    core = lax.axis_index(CORE).reshape(1)
    mine, other = sum_over_rows(gram(snapshots, core))
    basis = group_solve(core, mine, other, start_block, row_total)
    own = group_basis(basis, snapshots)
    joined = lax.all_gather(own, "grp", axis=0, tiled=True)
    mine, other = sum_over_rows(merge_partials(core, joined, test_block))
    return finish(core, mine, other, start_merge, joined, row_total)


def solution(mesh):
    finer = Mesh(
        mesh.devices.reshape(mesh.shape["grp"], 4, 8, 2), ("grp", "row_0", "row_1", "row_2")
    )
    placed = (P(ROW, "grp"), P(ROW, "grp"), P("grp", None), P())
    return jax.shard_map(
        on_device, mesh=finer, in_specs=placed, out_specs=P(ROW, "grp"), check_vma=False
    )
```

```python
import jax
import jax.numpy as jnp
from jax import lax
from jax.experimental import pallas as pl
from jax.experimental.pallas import tpu as pltpu
from jax.sharding import Mesh
from jax.sharding import PartitionSpec as P

ITERS = 6
ROW = ("row_0", "row_1", "row_2")
CHIPS = ("row_0", "row_1")
CORE = "row_2"
BLOCK = 128
VMEM = pl.BlockSpec(memory_space=pltpu.VMEM)
SMEM = pl.BlockSpec(memory_space=pltpu.SMEM)

NT = (((1,), (1,)), ((), ()))
NN = (((1,), (0,)), ((), ()))
TN = (((0,), (0,)), ((), ()))


def dot(left, right, dims):
    return lax.dot_general(left, right, dims, preferred_element_type=jnp.float32)


def parts(x, count):
    found = []
    for _ in range(count - 1):
        piece = x.astype(jnp.bfloat16)
        found.append(piece)
        x = x - piece.astype(jnp.float32)
    found.append(x.astype(jnp.bfloat16))
    return found


def dot_parts(left, right, dims):
    count = len(left)
    rows = left[0].shape[0]
    total = None
    for j in reversed(range(count)):
        stack = jnp.concatenate(left[: count - j], axis=0) if j < count - 1 else left[0]
        product = dot(stack, right[j], dims)
        for i in reversed(range(count - j)):
            piece = product[i * rows : (i + 1) * rows]
            total = piece if total is None else total + piece
    return total


def lower_inverse(matrix):
    size = matrix.shape[0]
    bands = size // 8
    sub = lax.broadcasted_iota(jnp.int32, (8, 2 * size), 0)
    lane = lax.broadcasted_iota(jnp.int32, (8, 2 * size), 1)
    wide = jnp.concatenate([matrix, jnp.zeros_like(matrix)], axis=1)
    work = [
        jnp.where(lane == size + 8 * b + sub, 1.0, wide[8 * b : 8 * b + 8]) for b in range(bands)
    ]

    def column(value, j):
        place = jnp.full(value.shape, j, jnp.int32)
        return jnp.take_along_axis(value, place, axis=1, mode="promise_in_bounds")

    def line(value, j):
        return jnp.broadcast_to(value[j : j + 1, :], value.shape)

    for b in range(bands):
        cols = {i: [column(work[i], 8 * b + j) for j in range(8)] for i in range(b, bands)}
        scale = None
        for j in range(8):
            pivot = line(cols[b][j], j)
            root = lax.rsqrt(pivot)
            inverse = root * root
            scale = root if scale is None else jnp.where(sub == j, root, scale)
            factor = jnp.where(sub > j, cols[b][j] * inverse, 0.0)
            ahead = {k: line(cols[b][k], j) for k in range(j + 1, 8)}
            pivot_row = line(work[b], j)
            for k in range(j + 1, 8):
                cols[b][k] = cols[b][k] - factor * ahead[k]
            work[b] = work[b] - factor * pivot_row
            for i in range(b + 1, bands):
                below = cols[i][j] * inverse
                for k in range(j + 1, 8):
                    cols[i][k] = cols[i][k] - below * ahead[k]
                work[i] = work[i] - below * pivot_row
        work[b] = work[b] * scale
    return jnp.concatenate(work, axis=0)[:, size:]


def orthonormal(rows):
    split = parts(rows, 3)
    return dot_parts(parts(lower_inverse(dot_parts(split, split, NT)), 3), split, NN)


def upper_pairs(count):
    return [(a, b) for a in range(count) for b in range(a, count)]


def cut(index):
    return slice(index * BLOCK, (index + 1) * BLOCK)


def gram_kernel(core_ref, x_ref, o_ref, held_ref, arrived, *sum_refs):
    steps, deep, width = held_ref.shape
    half = width // 2
    copies = [
        pltpu.make_async_copy(
            x_ref.at[pl.ds(n * deep, deep), :], held_ref.at[n], arrived.at[n]
        )
        for n in range(steps)
    ]
    for copy in copies:
        copy.start()
    left, right = slice(None, half), slice(half, None)
    for n, copy in enumerate(copies):
        copy.wait()
        high, low = parts(held_ref[n], 2)
        high_t, low_t = high.T, low.T
        found = [
            dot(high_t[left], high[:, left], NN) + dot(low_t[left], low[:, left], NN),
            dot(high_t[left], high[:, right], NN) + dot(low_t[left], low[:, right], NN),
            dot(high_t[right], high[:, right], NN) + dot(low_t[right], low[:, right], NN),
            dot(high_t[left], low[:, left], NN),
            dot(high_t[left], low[:, right], NN),
            dot(high_t[right], low[:, left], NN),
            dot(high_t[right], low[:, right], NN),
        ]
        for ref, value in zip(sum_refs, found):
            ref[...] = value if n == 0 else ref[...] + value
    aa, ab, bb, ll, lr, rl, rr = [ref[...] for ref in sum_refs]
    place = {(0, 0): aa + ll + ll.T, (0, 1): ab + lr + rl.T, (1, 1): bb + rr + rr.T}
    pairs = upper_pairs(width // BLOCK)
    held = len(pairs) // 2
    for n, (a, b) in enumerate(pairs):
        block = place[a // 2, b // 2][cut(a % 2), cut(b % 2)]
        o_ref[(n // held) ^ core_ref[0], cut(n % held), :] = block


def gram(snapshots, core):
    rows, width = snapshots.shape
    steps = 4
    held = len(upper_pairs(width // BLOCK)) // 2 * BLOCK
    return pl.pallas_call(
        gram_kernel,
        in_specs=[SMEM, pl.BlockSpec(memory_space=pl.ANY)],
        out_specs=VMEM,
        out_shape=jax.ShapeDtypeStruct((2, held, BLOCK), jnp.float32),
        scratch_shapes=[
            pltpu.VMEM((steps, rows // steps, width), jnp.float32),
            pltpu.SemaphoreType.DMA((steps,)),
        ]
        + [pltpu.VMEM((width // 2, width // 2), jnp.float32)] * 7,
        compiler_params=pltpu.CompilerParams(vmem_limit_bytes=48 * 2**20),
        name="gram",
    )(core, snapshots)


def in_order(core_ref, mine_ref, other_ref):
    first = core_ref[0] == 0
    mine, other = mine_ref[...], other_ref[...]
    return jnp.where(first, mine, other), jnp.where(first, other, mine)


def sweep(rows, gram_refs):
    split = parts(rows, 3)
    ahead = dot_parts(split, [ref[...] for ref in gram_refs], NN)
    return lower_inverse(dot_parts(split, split, NT)), ahead


def normalised(inverse, rows):
    return dot_parts(parts(inverse, 3), parts(rows, 3), NN)


def solve_kernel(row_total, core_ref, mine_ref, other_ref, start_ref, o_ref, next_ref, *gram_refs):
    width = gram_refs[0].shape[0]
    pairs = upper_pairs(width // BLOCK)
    held = len(pairs) // 2
    halves = in_order(core_ref, mine_ref, other_ref)
    for n, (a, b) in enumerate(pairs):
        block = halves[n // held][cut(n % held)] / row_total
        for ref, piece in zip(gram_refs, parts(block, 3)):
            ref[cut(a), cut(b)] = piece
        if a != b:
            for ref, piece in zip(gram_refs, parts(block.T, 3)):
                ref[cut(b), cut(a)] = piece
    next_ref[...] = start_ref[...].T

    def step(index, carry):
        next_ref[...] = normalised(*sweep(next_ref[...], gram_refs))
        return carry

    lax.fori_loop(0, ITERS, step, 0)
    o_ref[...] = orthonormal(next_ref[...])


def group_solve(core, mine, other, start, row_total):
    width, rank = start.shape
    return pl.pallas_call(
        lambda *refs: solve_kernel(row_total, *refs),
        in_specs=[SMEM, VMEM, VMEM, VMEM],
        out_specs=VMEM,
        out_shape=jax.ShapeDtypeStruct((rank, width), jnp.float32),
        scratch_shapes=[pltpu.VMEM((rank, width), jnp.float32)]
        + [pltpu.VMEM((width, width), jnp.bfloat16)] * 3,
        compiler_params=pltpu.CompilerParams(vmem_limit_bytes=32 * 2**20),
        name="group_solve",
    )(core, mine, other, start)


def basis_kernel(q_ref, x_ref, near_ref, far_ref):
    step = pl.program_id(0)
    half = pl.num_programs(0) // 2
    found = dot_parts(parts(q_ref[...], 2), parts(x_ref[...], 2), NT)

    @pl.when(step < half)
    def _():
        near_ref[...] = found

    @pl.when(step >= half)
    def _():
        far_ref[...] = found


def group_basis(basis, snapshots):
    rank, width = basis.shape
    rows = snapshots.shape[0]
    steps = 4
    deep = rows // steps
    half = steps // 2
    return pl.pallas_call(
        basis_kernel,
        grid=(steps,),
        in_specs=[
            pl.BlockSpec((rank, width), lambda i: (0, 0)),
            pl.BlockSpec((deep, width), lambda i: (i, 0)),
        ],
        out_specs=[
            pl.BlockSpec((rank, deep), lambda i: (0, jnp.minimum(i, half - 1))),
            pl.BlockSpec((rank, deep), lambda i: (0, jnp.maximum(i - half, 0))),
        ],
        out_shape=[jax.ShapeDtypeStruct((rank, rows // 2), jnp.float32)] * 2,
        compiler_params=pltpu.CompilerParams(
            dimension_semantics=("arbitrary",), vmem_limit_bytes=48 * 2**20
        ),
        name="group_basis",
    )(basis, snapshots)


def merge_kernel(place_ref, test_ref, *refs):
    joined_refs, o_ref = refs[:-1], refs[-1]
    count = len(joined_refs) // 2
    half = joined_refs[0].shape[1]
    merged, side = None, None
    for h in range(2):
        left = parts(jnp.concatenate([r[...] for r in joined_refs[h::2]], axis=0), 2)
        right = parts(test_ref[h * half : (h + 1) * half, :], 2)
        own = dot_parts(left, left, NT)
        other = dot_parts(left, right, NN)
        merged = own if merged is None else merged + own
        side = other if side is None else side + other
    blocks = [merged[cut(a), cut(b)] for a, b in upper_pairs(2)]
    blocks += [side[cut(a), :] for a in range(2)]
    pieces = [block[i * 64 : (i + 1) * 64] for block in blocks for i in range(2)]
    for n, piece in enumerate(pieces):
        o_ref[(n // 5) ^ place_ref[0], (n % 5) * 64 : (n % 5 + 1) * 64, :] = piece


def merge_partials(place, joined, test_block):
    return pl.pallas_call(
        merge_kernel,
        in_specs=[SMEM] + [VMEM] * (1 + len(joined)),
        out_specs=VMEM,
        out_shape=jax.ShapeDtypeStruct((2, 320, BLOCK), jnp.float32),
        compiler_params=pltpu.CompilerParams(vmem_limit_bytes=48 * 2**20),
        name="merge_partials",
    )(place, test_block, *joined)


def finish_kernel(row_total, place_ref, mine_ref, other_ref, start_ref, *refs):
    *joined_refs, o_ref, next_ref, high_ref, middle_ref, low_ref = refs
    gram_refs = [high_ref, middle_ref, low_ref]
    halves = in_order(place_ref, mine_ref, other_ref)
    pieces = [halves[n // 5][(n % 5) * 64 : (n % 5 + 1) * 64] for n in range(10)]
    blocks = [jnp.concatenate(pieces[2 * n : 2 * n + 2], axis=0) for n in range(5)]
    for (a, b), block in zip(upper_pairs(2), blocks[:3]):
        block = block / row_total
        for ref, piece in zip(gram_refs, parts(block, 3)):
            ref[cut(a), cut(b)] = piece
        if a != b:
            for ref, piece in zip(gram_refs, parts(block.T, 3)):
                ref[cut(b), cut(a)] = piece
    groups = start_ref.shape[0]
    turned = [start_ref[(place_ref[1] + k) % groups] for k in range(groups)]
    next_ref[...] = jnp.concatenate(turned, axis=0).T

    def step(index, carry):
        next_ref[...] = normalised(*sweep(next_ref[...], gram_refs))
        return carry

    lax.fori_loop(0, ITERS, step, 0)
    inverse, ahead = sweep(next_ref[...], gram_refs)
    coef = parts(normalised(inverse, next_ref[...]), 3)
    energy = dot_parts(parts(normalised(inverse, ahead), 3), coef, NT)
    coef = dot_parts(parts(lower_inverse(energy), 3), coef, NN)
    side = jnp.concatenate(blocks[3:], axis=0)
    test_coeffs = dot_parts(parts(coef, 3), parts(side, 3), NN)
    weight = dot_parts(parts(coef.T, 3), parts(test_coeffs, 3), NN) / row_total
    weight = parts(weight.T, 2)
    half = joined_refs[0].shape[1]
    deep = half // 2
    for n in range(4):
        here = slice(n % 2 * deep, (n % 2 + 1) * deep)
        joined = jnp.concatenate([r[:, here] for r in joined_refs[n // 2 :: 2]], axis=0)
        o_ref[n * deep : (n + 1) * deep, :] = dot_parts(weight, parts(joined, 2), NN).T


def finish(place, mine, other, start, joined, row_total):
    rank = start.shape[-1]
    wide = start.shape[0] * start.shape[1]
    rows = 2 * joined[0].shape[1]
    return pl.pallas_call(
        lambda *refs: finish_kernel(row_total, *refs),
        in_specs=[SMEM] + [VMEM] * (3 + len(joined)),
        out_specs=VMEM,
        out_shape=jax.ShapeDtypeStruct((rows, BLOCK), jnp.float32),
        scratch_shapes=[pltpu.VMEM((rank, wide), jnp.float32)]
        + [pltpu.VMEM((wide, wide), jnp.bfloat16)] * 3,
        compiler_params=pltpu.CompilerParams(vmem_limit_bytes=48 * 2**20),
        name="finish",
    )(place, mine, other, start, *joined)


def swap_cores(array):
    return lax.ppermute(array, CORE, [(0, 1), (1, 0)])


def sum_over_rows(halves):
    kept = halves[0] + swap_cores(halves[1])
    near, far = CHIPS
    lanes = lax.axis_size(near)
    cuts = kept.reshape(lanes, kept.shape[0] // lanes, BLOCK)
    own = jnp.sum(lax.all_to_all(cuts, near, 0, 0, tiled=True), axis=0)
    copies = jnp.broadcast_to(own, (lax.axis_size(far), *own.shape))
    own = jnp.sum(lax.all_to_all(copies, far, 0, 0, tiled=True), axis=0)
    copies = jnp.broadcast_to(own, (lanes, *own.shape))
    mine = lax.all_to_all(copies, near, 0, 0, tiled=True).reshape(kept.shape)
    return mine, swap_cores(mine)


def gathered_bases(near, far):
    groups = lax.axis_size("grp")
    down = [(i, (i - 1) % groups) for i in range(groups)]
    up = [(i, (i + 1) % groups) for i in range(groups)]
    next_near = lax.ppermute(near, "grp", down)
    last_far = lax.ppermute(far, "grp", up)
    next_far = lax.ppermute(far, "grp", down)
    last_near = lax.ppermute(near, "grp", up)
    across_near = lax.ppermute(next_near, "grp", down)
    across_far = lax.ppermute(last_far, "grp", up)
    return [near, far, next_near, next_far, across_near, across_far, last_near, last_far]


def on_device(snapshots, test_block, start_block, start_merge):
    row_total = snapshots.shape[0] * lax.axis_size(ROW)
    place = jnp.stack([lax.axis_index(CORE), lax.axis_index("grp")])
    groups = lax.axis_size("grp")
    mine, other = sum_over_rows(gram(snapshots, place))
    basis = group_solve(place, mine, other, start_block, row_total)
    joined = gathered_bases(*group_basis(basis, snapshots))
    mine, other = sum_over_rows(merge_partials(place, joined, test_block))
    start = start_merge.reshape(groups, start_merge.shape[0] // groups, start_merge.shape[1])
    return finish(place, mine, other, start, joined, row_total)


def solution(mesh):
    finer = Mesh(
        mesh.devices.reshape(mesh.shape["grp"], 4, 8, 2), ("grp", "row_0", "row_1", "row_2")
    )
    placed = (P(ROW, "grp"), P(ROW, "grp"), P("grp", None), P())
    return jax.shard_map(
        on_device, mesh=finer, in_specs=placed, out_specs=P(ROW, "grp"), check_vma=False
    )
```

```python
import jax
import jax.numpy as jnp
from jax import lax
from jax.experimental import pallas as pl
from jax.experimental.pallas import tpu as pltpu
from jax.sharding import Mesh
from jax.sharding import PartitionSpec as P

ITERS = 6
ROW = ("row_0", "row_1", "row_2")
CHIPS = ("row_0", "row_1")
CORE = "row_2"
BLOCK = 128
SHIFTS = (0, 1, 3, 2)
VMEM = pl.BlockSpec(memory_space=pltpu.VMEM)
SMEM = pl.BlockSpec(memory_space=pltpu.SMEM)

NT = (((1,), (1,)), ((), ()))
NN = (((1,), (0,)), ((), ()))
TN = (((0,), (0,)), ((), ()))


def dot(left, right, dims):
    return lax.dot_general(left, right, dims, preferred_element_type=jnp.float32)


def parts(x, count):
    found = []
    for _ in range(count - 1):
        piece = x.astype(jnp.bfloat16)
        found.append(piece)
        x = x - piece.astype(jnp.float32)
    found.append(x.astype(jnp.bfloat16))
    return found


def dot_parts(left, right, dims):
    count = len(left)
    rows = left[0].shape[0]
    total = None
    for j in reversed(range(count)):
        stack = jnp.concatenate(left[: count - j], axis=0) if j < count - 1 else left[0]
        product = dot(stack, right[j], dims)
        for i in reversed(range(count - j)):
            piece = product[i * rows : (i + 1) * rows]
            total = piece if total is None else total + piece
    return total


def lower_inverse(matrix):
    size = matrix.shape[0]
    bands = size // 8
    sub = lax.broadcasted_iota(jnp.int32, (8, 2 * size), 0)
    lane = lax.broadcasted_iota(jnp.int32, (8, 2 * size), 1)
    wide = jnp.concatenate([matrix, jnp.zeros_like(matrix)], axis=1)
    work = [
        jnp.where(lane == size + 8 * b + sub, 1.0, wide[8 * b : 8 * b + 8]) for b in range(bands)
    ]

    def column(value, j):
        place = jnp.full(value.shape, j, jnp.int32)
        return jnp.take_along_axis(value, place, axis=1, mode="promise_in_bounds")

    def line(value, j):
        return jnp.broadcast_to(value[j : j + 1, :], value.shape)

    diagonal = [column(work[0], j) for j in range(8)]
    for b in range(bands):
        cols = {i: [column(work[i], 8 * b + j) for j in range(8)] for i in range(b + 1, bands)}
        coming = [column(work[b + 1], 8 * b + 8 + k) for k in range(8)] if cols else None
        scale = None
        for j in range(8):
            pivot = line(diagonal[j], j)
            root = lax.rsqrt(pivot)
            inverse = root * root
            scale = root if scale is None else jnp.where(sub == j, root, scale)
            lower = jnp.where(sub > j, diagonal[j], 0.0)
            factor = lower * inverse
            ahead = {k: line(diagonal[k], j) for k in range(j + 1, 8)}
            pivot_row = line(work[b], j)
            for k in range(j + 1, 8):
                change = lower * ahead[k] * inverse if k == j + 1 else factor * ahead[k]
                diagonal[k] = diagonal[k] - change
            work[b] = work[b] - factor * pivot_row
            for i in range(b + 1, bands):
                below = cols[i][j] * inverse
                for k in range(j + 1, 8):
                    cols[i][k] = cols[i][k] - below * ahead[k]
                work[i] = work[i] - below * pivot_row
                if i == b + 1:
                    coming = [coming[k] - below * line(cols[i][j], k) for k in range(8)]
        work[b] = work[b] * scale
        diagonal = coming
    return jnp.concatenate(work, axis=0)[:, size:]


def orthonormal(rows):
    split = parts(rows, 3)
    return dot_parts(parts(lower_inverse(dot_parts(split, split, NT)), 3), split, NN)


def upper_pairs(count):
    return [(a, b) for a in range(count) for b in range(a, count)]


def cut(index):
    return slice(index * BLOCK, (index + 1) * BLOCK)


def gram_kernel(core_ref, x_ref, o_ref, held_ref, arrived, *sum_refs):
    steps, deep, width = held_ref.shape
    half = width // 2
    copies = [
        pltpu.make_async_copy(
            x_ref.at[pl.ds(n * deep, deep), :], held_ref.at[n], arrived.at[n]
        )
        for n in range(steps)
    ]
    for copy in copies:
        copy.start()
    left, right = slice(None, half), slice(half, None)
    for n, copy in enumerate(copies):
        copy.wait()
        high, low = parts(held_ref[n], 2)
        high_t, low_t = high.T, low.T
        found = [
            dot(high_t[left], high[:, left], NN) + dot(low_t[left], low[:, left], NN),
            dot(high_t[left], high[:, right], NN) + dot(low_t[left], low[:, right], NN),
            dot(high_t[right], high[:, right], NN) + dot(low_t[right], low[:, right], NN),
            dot(high_t[left], low[:, left], NN),
            dot(high_t[left], low[:, right], NN),
            dot(high_t[right], low[:, left], NN),
            dot(high_t[right], low[:, right], NN),
        ]
        for ref, value in zip(sum_refs, found):
            ref[...] = value if n == 0 else ref[...] + value
    aa, ab, bb, ll, lr, rl, rr = [ref[...] for ref in sum_refs]
    place = {(0, 0): aa + ll + ll.T, (0, 1): ab + lr + rl.T, (1, 1): bb + rr + rr.T}
    pairs = upper_pairs(width // BLOCK)
    held = len(pairs) // 2
    for n, (a, b) in enumerate(pairs):
        block = place[a // 2, b // 2][cut(a % 2), cut(b % 2)]
        o_ref[(n // held) ^ core_ref[0], cut(n % held), :] = block


def gram(snapshots, core):
    rows, width = snapshots.shape
    steps = 4
    held = len(upper_pairs(width // BLOCK)) // 2 * BLOCK
    return pl.pallas_call(
        gram_kernel,
        in_specs=[SMEM, pl.BlockSpec(memory_space=pl.ANY)],
        out_specs=VMEM,
        out_shape=jax.ShapeDtypeStruct((2, held, BLOCK), jnp.float32),
        scratch_shapes=[
            pltpu.VMEM((steps, rows // steps, width), jnp.float32),
            pltpu.SemaphoreType.DMA((steps,)),
        ]
        + [pltpu.VMEM((width // 2, width // 2), jnp.float32)] * 7,
        compiler_params=pltpu.CompilerParams(vmem_limit_bytes=48 * 2**20),
        name="gram",
    )(core, snapshots)


def in_order(core_ref, mine_ref, other_ref):
    first = core_ref[0] == 0
    mine, other = mine_ref[...], other_ref[...]
    return jnp.where(first, mine, other), jnp.where(first, other, mine)


def sweep(rows, gram_refs):
    split = parts(rows, 3)
    ahead = dot_parts(split, [ref[...] for ref in gram_refs], NN)
    return lower_inverse(dot_parts(split, split, NT)), ahead


def normalised(inverse, rows):
    return dot_parts(parts(inverse, 3), parts(rows, 3), NN)


def solve_kernel(row_total, core_ref, mine_ref, other_ref, start_ref, o_ref, next_ref, *gram_refs):
    width = gram_refs[0].shape[0]
    pairs = upper_pairs(width // BLOCK)
    held = len(pairs) // 2
    halves = in_order(core_ref, mine_ref, other_ref)
    for n, (a, b) in enumerate(pairs):
        block = halves[n // held][cut(n % held)] / row_total
        for ref, piece in zip(gram_refs, parts(block, 3)):
            ref[cut(a), cut(b)] = piece
        if a != b:
            for ref, piece in zip(gram_refs, parts(block.T, 3)):
                ref[cut(b), cut(a)] = piece
    next_ref[...] = start_ref[...].T

    def step(index, carry):
        next_ref[...] = normalised(*sweep(next_ref[...], gram_refs))
        return carry

    lax.fori_loop(0, ITERS, step, 0)
    o_ref[...] = orthonormal(next_ref[...])


def group_solve(core, mine, other, start, row_total):
    width, rank = start.shape
    return pl.pallas_call(
        lambda *refs: solve_kernel(row_total, *refs),
        in_specs=[SMEM, VMEM, VMEM, VMEM],
        out_specs=VMEM,
        out_shape=jax.ShapeDtypeStruct((rank, width), jnp.float32),
        scratch_shapes=[pltpu.VMEM((rank, width), jnp.float32)]
        + [pltpu.VMEM((width, width), jnp.bfloat16)] * 3,
        compiler_params=pltpu.CompilerParams(vmem_limit_bytes=32 * 2**20),
        name="group_solve",
    )(core, mine, other, start)


def basis_kernel(q_ref, x_ref, near_ref, far_ref):
    step = pl.program_id(0)
    half = pl.num_programs(0) // 2
    found = dot_parts(parts(q_ref[...], 2), parts(x_ref[...], 2), NT)

    @pl.when(step < half)
    def _():
        near_ref[...] = found

    @pl.when(step >= half)
    def _():
        far_ref[...] = found


def group_basis(basis, snapshots):
    rank, width = basis.shape
    rows = snapshots.shape[0]
    steps = 4
    deep = rows // steps
    half = steps // 2
    return pl.pallas_call(
        basis_kernel,
        grid=(steps,),
        in_specs=[
            pl.BlockSpec((rank, width), lambda i: (0, 0)),
            pl.BlockSpec((deep, width), lambda i: (i, 0)),
        ],
        out_specs=[
            pl.BlockSpec((rank, deep), lambda i: (0, jnp.minimum(i, half - 1))),
            pl.BlockSpec((rank, deep), lambda i: (0, jnp.maximum(i - half, 0))),
        ],
        out_shape=[jax.ShapeDtypeStruct((rank, rows // 2), jnp.float32)] * 2,
        compiler_params=pltpu.CompilerParams(
            dimension_semantics=("arbitrary",), vmem_limit_bytes=48 * 2**20
        ),
        name="group_basis",
    )(basis, snapshots)


def stacked(refs, h):
    return jnp.concatenate([ref[...] for ref in refs[h::2]], axis=0)


def merge_near_kernel(test_ref, *refs):
    *joined_refs, merged_ref, side_ref = refs
    half = joined_refs[0].shape[1]
    merged, side = None, None
    for h in range(2):
        left = parts(stacked(joined_refs, h), 2)
        right = parts(test_ref[h * half : (h + 1) * half, :], 2)
        own = dot_parts(left, left, NT)
        other = dot_parts(left, right, NN)
        merged = own if merged is None else merged + own
        side = other if side is None else side + other
    merged_ref[...] = merged
    side_ref[...] = side


def merge_near(joined, test_block):
    wide = len(joined) // 2 * joined[0].shape[0]
    return pl.pallas_call(
        merge_near_kernel,
        in_specs=[VMEM] * (1 + len(joined)),
        out_specs=[VMEM, VMEM],
        out_shape=[
            jax.ShapeDtypeStruct((wide, wide), jnp.float32),
            jax.ShapeDtypeStruct((wide, BLOCK), jnp.float32),
        ],
        compiler_params=pltpu.CompilerParams(vmem_limit_bytes=48 * 2**20),
        name="merge_near",
    )(test_block, *joined)


def merge_kernel(place_ref, merged_ref, side_ref, test_ref, *refs):
    *joined_refs, o_ref = refs
    half = joined_refs[0].shape[1]
    rank = joined_refs[0].shape[0]
    cross, last = None, None
    for h in range(2):
        left = parts(stacked(joined_refs, h), 2)
        across = [piece[-rank:] for piece in left]
        right = parts(test_ref[h * half : (h + 1) * half, :], 2)
        own = dot_parts(left, across, NT)
        other = dot_parts(across, right, NN)
        cross = own if cross is None else cross + own
        last = other if last is None else last + other
    merged, side = merged_ref[...], side_ref[...]
    blocks = [
        merged[:BLOCK, :BLOCK],
        jnp.concatenate([merged[:BLOCK, BLOCK:], cross[:BLOCK]], axis=1),
        jnp.concatenate(
            [jnp.concatenate([merged[BLOCK:, BLOCK:], cross[BLOCK:-rank].T], axis=0), cross[BLOCK:]],
            axis=1,
        ),
    ]
    side = jnp.concatenate([side, last], axis=0)
    blocks += [side[cut(a), :] for a in range(2)]
    pieces = [block[i * 64 : (i + 1) * 64] for block in blocks for i in range(2)]
    for n, piece in enumerate(pieces):
        o_ref[(n // 5) ^ place_ref[0], (n % 5) * 64 : (n % 5 + 1) * 64, :] = piece


def merge_partials(place, joined, test_block):
    return pl.pallas_call(
        merge_kernel,
        in_specs=[SMEM] + [VMEM] * (3 + len(joined)),
        out_specs=VMEM,
        out_shape=jax.ShapeDtypeStruct((2, 320, BLOCK), jnp.float32),
        compiler_params=pltpu.CompilerParams(vmem_limit_bytes=48 * 2**20),
        name="merge_partials",
    )(place, *merge_near(joined[:-2], test_block), test_block, *joined)


def finish_kernel(row_total, place_ref, mine_ref, other_ref, start_ref, *refs):
    *joined_refs, o_ref, next_ref, high_ref, middle_ref, low_ref = refs
    gram_refs = [high_ref, middle_ref, low_ref]
    halves = in_order(place_ref, mine_ref, other_ref)
    pieces = [halves[n // 5][(n % 5) * 64 : (n % 5 + 1) * 64] for n in range(10)]
    blocks = [jnp.concatenate(pieces[2 * n : 2 * n + 2], axis=0) for n in range(5)]
    for (a, b), block in zip(upper_pairs(2), blocks[:3]):
        block = block / row_total
        for ref, piece in zip(gram_refs, parts(block, 3)):
            ref[cut(a), cut(b)] = piece
        if a != b:
            for ref, piece in zip(gram_refs, parts(block.T, 3)):
                ref[cut(b), cut(a)] = piece
    groups = start_ref.shape[0]
    turned = [start_ref[(place_ref[1] + k) % groups] for k in SHIFTS]
    next_ref[...] = jnp.concatenate(turned, axis=0).T

    def step(index, carry):
        next_ref[...] = normalised(*sweep(next_ref[...], gram_refs))
        return carry

    lax.fori_loop(0, ITERS, step, 0)
    inverse, ahead = sweep(next_ref[...], gram_refs)
    coef = parts(normalised(inverse, next_ref[...]), 3)
    energy = dot_parts(parts(normalised(inverse, ahead), 3), coef, NT)
    coef = dot_parts(parts(lower_inverse(energy), 3), coef, NN)
    side = jnp.concatenate(blocks[3:], axis=0)
    test_coeffs = dot_parts(parts(coef, 3), parts(side, 3), NN)
    weight = dot_parts(parts(coef.T, 3), parts(test_coeffs, 3), NN) / row_total
    weight = parts(weight.T, 2)
    half = joined_refs[0].shape[1]
    deep = half // 2
    for n in range(4):
        here = slice(n % 2 * deep, (n % 2 + 1) * deep)
        joined = jnp.concatenate([r[:, here] for r in joined_refs[n // 2 :: 2]], axis=0)
        o_ref[n * deep : (n + 1) * deep, :] = dot_parts(weight, parts(joined, 2), NN).T


def finish(place, mine, other, start, joined, row_total):
    rank = start.shape[-1]
    wide = start.shape[0] * start.shape[1]
    rows = 2 * joined[0].shape[1]
    return pl.pallas_call(
        lambda *refs: finish_kernel(row_total, *refs),
        in_specs=[SMEM] + [VMEM] * (3 + len(joined)),
        out_specs=VMEM,
        out_shape=jax.ShapeDtypeStruct((rows, BLOCK), jnp.float32),
        scratch_shapes=[pltpu.VMEM((rank, wide), jnp.float32)]
        + [pltpu.VMEM((wide, wide), jnp.bfloat16)] * 3,
        compiler_params=pltpu.CompilerParams(vmem_limit_bytes=48 * 2**20),
        name="finish",
    )(place, mine, other, start, *joined)


def swap_cores(array):
    return lax.ppermute(array, CORE, [(0, 1), (1, 0)])


def reduced(array, axis):
    length = lax.axis_size(axis)
    cuts = array.reshape(length, array.shape[0] // length, BLOCK)
    return jnp.sum(lax.all_to_all(cuts, axis, 0, 0, tiled=True), axis=0)


def spread(array, axis):
    copies = jnp.broadcast_to(array, (lax.axis_size(axis), *array.shape))
    return lax.all_to_all(copies, axis, 0, 0, tiled=True)


def sum_over_rows(halves):
    near, far = CHIPS
    kept = halves[0] + swap_cores(halves[1])
    own = reduced(kept, near)
    if own.shape[0] > 100:
        own = spread(reduced(own, far), far).reshape(own.shape)
    else:
        own = jnp.sum(spread(own, far), axis=0)
    mine = spread(own, near).reshape(kept.shape)
    return mine, swap_cores(mine)


def gathered_bases(near, far):
    groups = lax.axis_size("grp")
    down = [(i, (i - 1) % groups) for i in range(groups)]
    up = [(i, (i + 1) % groups) for i in range(groups)]
    next_near = lax.ppermute(near, "grp", down)
    last_far = lax.ppermute(far, "grp", up)
    next_far = lax.ppermute(far, "grp", down)
    last_near = lax.ppermute(near, "grp", up)
    across_near = lax.ppermute(next_near, "grp", down)
    across_far = lax.ppermute(last_far, "grp", up)
    return [near, far, next_near, next_far, last_near, last_far, across_near, across_far]


def on_device(snapshots, test_block, start_block, start_merge):
    row_total = snapshots.shape[0] * lax.axis_size(ROW)
    place = jnp.stack([lax.axis_index(CORE), lax.axis_index("grp")])
    groups = lax.axis_size("grp")
    mine, other = sum_over_rows(gram(snapshots, place))
    basis = group_solve(place, mine, other, start_block, row_total)
    joined = gathered_bases(*group_basis(basis, snapshots))
    mine, other = sum_over_rows(merge_partials(place, joined, test_block))
    start = start_merge.reshape(groups, start_merge.shape[0] // groups, start_merge.shape[1])
    return finish(place, mine, other, start, joined, row_total)


def solution(mesh):
    finer = Mesh(
        mesh.devices.reshape(mesh.shape["grp"], 4, 8, 2), ("grp", "row_0", "row_1", "row_2")
    )
    placed = (P(ROW, "grp"), P(ROW, "grp"), P("grp", None), P())
    return jax.shard_map(
        on_device, mesh=finer, in_specs=placed, out_specs=P(ROW, "grp"), check_vma=False
    )
```

```python
import jax
import jax.numpy as jnp
from jax import lax
from jax.experimental import pallas as pl
from jax.experimental.pallas import tpu as pltpu
from jax.sharding import Mesh
from jax.sharding import PartitionSpec as P

ITERS = 6
ROW = ("row_0", "row_1", "row_2")
CHIPS = ("row_0", "row_1")
CORE = "row_2"
BLOCK = 128
SHIFTS = (0, 1, 3, 2)
HBM = pl.BlockSpec(memory_space=pltpu.HBM)
VMEM = pl.BlockSpec(memory_space=pltpu.VMEM)
SMEM = pl.BlockSpec(memory_space=pltpu.SMEM)

NT = (((1,), (1,)), ((), ()))
NN = (((1,), (0,)), ((), ()))
TN = (((0,), (0,)), ((), ()))


def dot(left, right, dims):
    return lax.dot_general(left, right, dims, preferred_element_type=jnp.float32)


def parts(x, count):
    found = []
    for _ in range(count - 1):
        piece = x.astype(jnp.bfloat16)
        found.append(piece)
        x = x - piece.astype(jnp.float32)
    found.append(x.astype(jnp.bfloat16))
    return found


def dot_parts(left, right, dims):
    count = len(left)
    rows = left[0].shape[0]
    total = None
    for j in reversed(range(count)):
        stack = jnp.concatenate(left[: count - j], axis=0) if j < count - 1 else left[0]
        product = dot(stack, right[j], dims)
        for i in reversed(range(count - j)):
            piece = product[i * rows : (i + 1) * rows]
            total = piece if total is None else total + piece
    return total


def lower_inverse(matrix):
    size = matrix.shape[0]
    bands = size // 8
    sub = lax.broadcasted_iota(jnp.int32, (8, 2 * size), 0)
    lane = lax.broadcasted_iota(jnp.int32, (8, 2 * size), 1)
    wide = jnp.concatenate([matrix, jnp.zeros_like(matrix)], axis=1)
    work = [
        jnp.where(lane == size + 8 * b + sub, 1.0, wide[8 * b : 8 * b + 8]) for b in range(bands)
    ]

    def column(value, j):
        place = jnp.full(value.shape, j, jnp.int32)
        return jnp.take_along_axis(value, place, axis=1, mode="promise_in_bounds")

    def line(value, j):
        return jnp.broadcast_to(value[j : j + 1, :], value.shape)

    diagonal = [column(work[0], j) for j in range(8)]
    for b in range(bands):
        cols = {i: [column(work[i], 8 * b + j) for j in range(8)] for i in range(b + 1, bands)}
        coming = [column(work[b + 1], 8 * b + 8 + k) for k in range(8)] if cols else None
        scale = None
        for j in range(8):
            pivot = line(diagonal[j], j)
            root = lax.rsqrt(pivot)
            inverse = root * root
            scale = root if scale is None else jnp.where(sub == j, root, scale)
            lower = jnp.where(sub > j, diagonal[j], 0.0)
            factor = lower * inverse
            ahead = {k: line(diagonal[k], j) for k in range(j + 1, 8)}
            pivot_row = line(work[b], j)
            for k in range(j + 1, 8):
                change = lower * ahead[k] * inverse if k == j + 1 else factor * ahead[k]
                diagonal[k] = diagonal[k] - change
            work[b] = work[b] - factor * pivot_row
            for i in range(b + 1, bands):
                below = cols[i][j] * inverse
                for k in range(j + 1, 8):
                    cols[i][k] = cols[i][k] - below * ahead[k]
                work[i] = work[i] - below * pivot_row
                if i == b + 1:
                    coming = [coming[k] - below * line(cols[i][j], k) for k in range(8)]
        work[b] = work[b] * scale
        diagonal = coming
    return jnp.concatenate(work, axis=0)[:, size:]


def orthonormal(rows):
    split = parts(rows, 3)
    return dot_parts(parts(lower_inverse(dot_parts(split, split, NT)), 3), split, NN)


def upper_pairs(count):
    return [(a, b) for a in range(count) for b in range(a, count)]


def cut(index):
    return slice(index * BLOCK, (index + 1) * BLOCK)


def gram_kernel(core_ref, x_ref, o_ref, held_ref, arrived, *sum_refs):
    steps, deep, width = held_ref.shape
    half = width // 2
    copies = [
        pltpu.make_async_copy(
            x_ref.at[pl.ds(n * deep, deep), :], held_ref.at[n], arrived.at[n]
        )
        for n in range(steps)
    ]
    for copy in copies:
        copy.start()
    left, right = slice(None, half), slice(half, None)
    for n, copy in enumerate(copies):
        copy.wait()
        high, low = parts(held_ref[n], 2)
        high_t = high.T
        found = [
            dot(high_t[left], high[:, left], NN),
            dot(high_t[left], high[:, right], NN),
            dot(high_t[right], high[:, right], NN),
            dot(high_t[left], low[:, left], NN),
            dot(high_t[left], low[:, right], NN),
            dot(high_t[right], low[:, left], NN),
            dot(high_t[right], low[:, right], NN),
        ]
        for ref, value in zip(sum_refs, found):
            ref[...] = value if n == 0 else ref[...] + value
    aa, ab, bb, ll, lr, rl, rr = [ref[...] for ref in sum_refs]
    place = {(0, 0): aa + ll + ll.T, (0, 1): ab + lr + rl.T, (1, 1): bb + rr + rr.T}
    pairs = upper_pairs(width // BLOCK)
    held = len(pairs) // 2
    for n, (a, b) in enumerate(pairs):
        block = place[a // 2, b // 2][cut(a % 2), cut(b % 2)]
        o_ref[(n // held) ^ core_ref[0], cut(n % held), :] = block


def gram(snapshots, core):
    rows, width = snapshots.shape
    steps = 4
    held = len(upper_pairs(width // BLOCK)) // 2 * BLOCK
    return pl.pallas_call(
        gram_kernel,
        in_specs=[SMEM, HBM],
        out_specs=VMEM,
        out_shape=jax.ShapeDtypeStruct((2, held, BLOCK), jnp.float32),
        scratch_shapes=[
            pltpu.VMEM((steps, rows // steps, width), jnp.float32),
            pltpu.SemaphoreType.DMA((steps,)),
        ]
        + [pltpu.VMEM((width // 2, width // 2), jnp.float32)] * 7,
        compiler_params=pltpu.CompilerParams(vmem_limit_bytes=48 * 2**20),
        name="gram",
    )(core, snapshots)


def in_order(core_ref, mine_ref, other_ref):
    first = core_ref[0] == 0
    mine, other = mine_ref[...], other_ref[...]
    return jnp.where(first, mine, other), jnp.where(first, other, mine)


def sweep(rows, gram_refs):
    split = parts(rows, 3)
    ahead = dot_parts(split, [ref[...] for ref in gram_refs], NN)
    return lower_inverse(dot_parts(split, split, NT)), ahead


def normalised(inverse, rows):
    return dot_parts(parts(inverse, 3), parts(rows, 3), NN)


def solve_kernel(row_total, core_ref, mine_ref, other_ref, start_ref, o_ref, next_ref, *gram_refs):
    width = gram_refs[0].shape[0]
    pairs = upper_pairs(width // BLOCK)
    held = len(pairs) // 2
    halves = in_order(core_ref, mine_ref, other_ref)
    for n, (a, b) in enumerate(pairs):
        block = halves[n // held][cut(n % held)] / row_total
        for ref, piece in zip(gram_refs, parts(block, 3)):
            ref[cut(a), cut(b)] = piece
        if a != b:
            for ref, piece in zip(gram_refs, parts(block.T, 3)):
                ref[cut(b), cut(a)] = piece
    next_ref[...] = start_ref[...].T

    def step(index, carry):
        next_ref[...] = normalised(*sweep(next_ref[...], gram_refs))
        return carry

    lax.fori_loop(0, ITERS, step, 0)
    o_ref[...] = orthonormal(next_ref[...])


def group_solve(core, mine, other, start, row_total):
    width, rank = start.shape
    return pl.pallas_call(
        lambda *refs: solve_kernel(row_total, *refs),
        in_specs=[SMEM, VMEM, VMEM, VMEM],
        out_specs=VMEM,
        out_shape=jax.ShapeDtypeStruct((rank, width), jnp.float32),
        scratch_shapes=[pltpu.VMEM((rank, width), jnp.float32)]
        + [pltpu.VMEM((width, width), jnp.bfloat16)] * 3,
        compiler_params=pltpu.CompilerParams(vmem_limit_bytes=32 * 2**20),
        name="group_solve",
    )(core, mine, other, start)


def group_basis(basis, snapshots, half):
    rank = basis.shape[0]
    rows = snapshots.shape[0]
    deep = rows // 4

    def kernel(q_ref, x_ref, o_ref, held_ref, arrived):
        copies = [
            pltpu.make_async_copy(
                x_ref.at[pl.ds((half * 2 + n) * deep, deep), :], held_ref.at[n], arrived.at[n]
            )
            for n in range(2)
        ]
        for copy in copies:
            copy.start()
        left = parts(q_ref[...], 2)
        for n, copy in enumerate(copies):
            copy.wait()
            right = parts(held_ref[n], 2)
            o_ref[:, n * deep : (n + 1) * deep] = dot_parts(left, right, NT)

    return pl.pallas_call(
        kernel,
        in_specs=[VMEM, HBM],
        out_specs=VMEM,
        out_shape=jax.ShapeDtypeStruct((rank, rows // 2), jnp.float32),
        scratch_shapes=[
            pltpu.VMEM((2, deep, snapshots.shape[1]), jnp.float32),
            pltpu.SemaphoreType.DMA((2,)),
        ],
        compiler_params=pltpu.CompilerParams(vmem_limit_bytes=48 * 2**20),
        name="group_basis",
    )(basis, snapshots)


def stacked(refs, h):
    return jnp.concatenate([ref[...] for ref in refs[h::2]], axis=0)


def merge_near_kernel(test_ref, *refs):
    *joined_refs, merged_ref, side_ref = refs
    half = joined_refs[0].shape[1]
    merged, side = None, None
    for h in range(2):
        left = parts(stacked(joined_refs, h), 2)
        right = parts(test_ref[h * half : (h + 1) * half, :], 2)
        own = dot_parts(left, left, NT)
        other = dot_parts(left, right, NN)
        merged = own if merged is None else merged + own
        side = other if side is None else side + other
    merged_ref[...] = merged
    side_ref[...] = side


def merge_near(joined, test_block):
    wide = len(joined) // 2 * joined[0].shape[0]
    return pl.pallas_call(
        merge_near_kernel,
        in_specs=[VMEM] * (1 + len(joined)),
        out_specs=[VMEM, VMEM],
        out_shape=[
            jax.ShapeDtypeStruct((wide, wide), jnp.float32),
            jax.ShapeDtypeStruct((wide, BLOCK), jnp.float32),
        ],
        compiler_params=pltpu.CompilerParams(vmem_limit_bytes=28 * 2**20),
        name="merge_near",
    )(test_block, *joined)


def merge_kernel(place_ref, merged_ref, side_ref, test_ref, *refs):
    *all_refs, o_ref = refs
    joined_refs, across_refs = all_refs[:-4], all_refs[-4:]
    rank, deep = across_refs[0].shape
    cross, last = None, None
    for n in range(4):
        here = slice(n % 2 * deep, (n % 2 + 1) * deep)
        pieces = [ref[:, here] for ref in joined_refs[n // 2 :: 2]] + [across_refs[n][...]]
        left = parts(jnp.concatenate(pieces, axis=0), 2)
        across = [piece[-rank:] for piece in left]
        right = parts(test_ref[n * deep : (n + 1) * deep, :], 2)
        own = dot_parts(left, across, NT)
        other = dot_parts(across, right, NN)
        cross = own if cross is None else cross + own
        last = other if last is None else last + other
    merged, side = merged_ref[...], side_ref[...]
    blocks = [
        merged[:BLOCK, :BLOCK],
        jnp.concatenate([merged[:BLOCK, BLOCK:], cross[:BLOCK]], axis=1),
        jnp.concatenate(
            [jnp.concatenate([merged[BLOCK:, BLOCK:], cross[BLOCK:-rank].T], axis=0), cross[BLOCK:]],
            axis=1,
        ),
    ]
    side = jnp.concatenate([side, last], axis=0)
    blocks += [side[cut(a), :] for a in range(2)]
    pieces = [block[i * 64 : (i + 1) * 64] for block in blocks for i in range(2)]
    for n, piece in enumerate(pieces):
        o_ref[(n // 5) ^ place_ref[0], (n % 5) * 64 : (n % 5 + 1) * 64, :] = piece


def merge_partials(place, joined, across, test_block):
    return pl.pallas_call(
        merge_kernel,
        in_specs=[SMEM] + [VMEM] * (3 + len(joined) + len(across)),
        out_specs=VMEM,
        out_shape=jax.ShapeDtypeStruct((2, 320, BLOCK), jnp.float32),
        compiler_params=pltpu.CompilerParams(vmem_limit_bytes=28 * 2**20),
        name="merge_partials",
    )(place, *merge_near(joined, test_block), test_block, *joined, *across)


def finish_kernel(row_total, place_ref, mine_ref, other_ref, start_ref, *refs):
    *joined_refs, o_ref, next_ref, high_ref, middle_ref, low_ref = refs
    gram_refs = [high_ref, middle_ref, low_ref]
    halves = in_order(place_ref, mine_ref, other_ref)
    pieces = [halves[n // 5][(n % 5) * 64 : (n % 5 + 1) * 64] for n in range(10)]
    blocks = [jnp.concatenate(pieces[2 * n : 2 * n + 2], axis=0) for n in range(5)]
    for (a, b), block in zip(upper_pairs(2), blocks[:3]):
        block = block / row_total
        for ref, piece in zip(gram_refs, parts(block, 3)):
            ref[cut(a), cut(b)] = piece
        if a != b:
            for ref, piece in zip(gram_refs, parts(block.T, 3)):
                ref[cut(b), cut(a)] = piece
    groups = start_ref.shape[0]
    turned = [start_ref[(place_ref[1] + k) % groups] for k in SHIFTS]
    next_ref[...] = jnp.concatenate(turned, axis=0).T

    def step(index, carry):
        next_ref[...] = normalised(*sweep(next_ref[...], gram_refs))
        return carry

    lax.fori_loop(0, ITERS, step, 0)
    inverse, ahead = sweep(next_ref[...], gram_refs)
    coef = parts(normalised(inverse, next_ref[...]), 3)
    energy = dot_parts(parts(normalised(inverse, ahead), 3), coef, NT)
    coef = dot_parts(parts(lower_inverse(energy), 3), coef, NN)
    side = jnp.concatenate(blocks[3:], axis=0)
    test_coeffs = dot_parts(parts(coef, 3), parts(side, 3), NN)
    weight = dot_parts(parts(coef.T, 3), parts(test_coeffs, 3), NN) / row_total
    weight = parts(weight.T, 2)
    across_refs = joined_refs[-4:]
    deep = across_refs[0].shape[1]
    for n in range(4):
        here = slice(n % 2 * deep, (n % 2 + 1) * deep)
        bases = [ref[:, here] for ref in joined_refs[:-4][n // 2 :: 2]] + [across_refs[n][...]]
        joined = jnp.concatenate(bases, axis=0)
        o_ref[n * deep : (n + 1) * deep, :] = dot_parts(weight, parts(joined, 2), NN).T


def finish(place, mine, other, start, joined, across, row_total):
    rank = start.shape[-1]
    wide = start.shape[0] * start.shape[1]
    rows = 2 * joined[0].shape[1]
    return pl.pallas_call(
        lambda *refs: finish_kernel(row_total, *refs),
        in_specs=[SMEM] + [VMEM] * (3 + len(joined) + len(across)),
        out_specs=VMEM,
        out_shape=jax.ShapeDtypeStruct((rows, BLOCK), jnp.float32),
        scratch_shapes=[pltpu.VMEM((rank, wide), jnp.float32)]
        + [pltpu.VMEM((wide, wide), jnp.bfloat16)] * 3,
        compiler_params=pltpu.CompilerParams(vmem_limit_bytes=28 * 2**20),
        name="finish",
    )(place, mine, other, start, *joined, *across)


def swap_cores(array):
    return lax.ppermute(array, CORE, [(0, 1), (1, 0)])


def reduced(array, axis):
    length = lax.axis_size(axis)
    cuts = array.reshape(length, array.shape[0] // length, BLOCK)
    return jnp.sum(lax.all_to_all(cuts, axis, 0, 0, tiled=True), axis=0)


def spread(array, axis):
    copies = jnp.broadcast_to(array, (lax.axis_size(axis), *array.shape))
    return lax.all_to_all(copies, axis, 0, 0, tiled=True)


def sum_over_rows(halves, staged):
    kept = halves[0] + swap_cores(halves[1])
    if staged:
        near, far = CHIPS
        mine = spread(jnp.sum(spread(reduced(kept, near), far), axis=0), near)
    else:
        mine = spread(reduced(kept, CHIPS), CHIPS)
    mine = mine.reshape(kept.shape)
    return mine, swap_cores(mine)


def gathered_bases(near, far):
    groups = lax.axis_size("grp")
    down = [(i, (i - 1) % groups) for i in range(groups)]
    up = [(i, (i + 1) % groups) for i in range(groups)]
    half = near.shape[1] // 2
    next_near = lax.ppermute(near, "grp", down)
    last_near = lax.ppermute(near, "grp", up)
    next_far = lax.ppermute(far, "grp", down)
    last_far = lax.ppermute(far, "grp", up)
    across = [
        lax.ppermute(next_near[:, :half], "grp", down),
        lax.ppermute(last_near[:, half:], "grp", up),
        lax.ppermute(next_far[:, :half], "grp", down),
        lax.ppermute(last_far[:, half:], "grp", up),
    ]
    return [near, far, next_near, next_far, last_near, last_far], across


def on_device(snapshots, test_block, start_block, start_merge):
    row_total = snapshots.shape[0] * lax.axis_size(ROW)
    place = jnp.stack([lax.axis_index(CORE), lax.axis_index("grp")])
    groups = lax.axis_size("grp")
    mine, other = sum_over_rows(gram(snapshots, place), False)
    basis = group_solve(place, mine, other, start_block, row_total)
    joined, across = gathered_bases(*[group_basis(basis, snapshots, h) for h in range(2)])
    mine, other = sum_over_rows(merge_partials(place, joined, across, test_block), True)
    start = start_merge.reshape(groups, start_merge.shape[0] // groups, start_merge.shape[1])
    return finish(place, mine, other, start, joined, across, row_total)


def solution(mesh):
    finer = Mesh(
        mesh.devices.reshape(mesh.shape["grp"], 4, 8, 2), ("grp", "row_0", "row_1", "row_2")
    )
    placed = (P(ROW, "grp"), P(ROW, "grp"), P("grp", None), P())
    return jax.shard_map(
        on_device, mesh=finer, in_specs=placed, out_specs=P(ROW, "grp"), check_vma=False
    )
```

```python
import jax
import jax.numpy as jnp
from jax import lax
from jax.experimental import pallas as pl
from jax.experimental.pallas import tpu as pltpu
from jax.sharding import Mesh
from jax.sharding import PartitionSpec as P

ITERS = 6
ROW = ("row_0", "row_1", "row_2")
CHIPS = ("row_0", "row_1")
CORE = "row_2"
BLOCK = 128
SHIFTS = (0, 1, 3, 2)
HBM = pl.BlockSpec(memory_space=pltpu.HBM)
VMEM = pl.BlockSpec(memory_space=pltpu.VMEM)
SMEM = pl.BlockSpec(memory_space=pltpu.SMEM)

NT = (((1,), (1,)), ((), ()))
NN = (((1,), (0,)), ((), ()))
TN = (((0,), (0,)), ((), ()))


def dot(left, right, dims):
    return lax.dot_general(left, right, dims, preferred_element_type=jnp.float32)


def parts(x, count):
    found = []
    for _ in range(count - 1):
        piece = x.astype(jnp.bfloat16)
        found.append(piece)
        x = x - piece.astype(jnp.float32)
    found.append(x.astype(jnp.bfloat16))
    return found


def dot_parts(left, right, dims):
    count = len(left)
    rows = left[0].shape[0]
    total = None
    for j in reversed(range(count)):
        stack = jnp.concatenate(left[: count - j], axis=0) if j < count - 1 else left[0]
        product = dot(stack, right[j], dims)
        for i in reversed(range(count - j)):
            piece = product[i * rows : (i + 1) * rows]
            total = piece if total is None else total + piece
    return total


def lower_inverse(matrix):
    size = matrix.shape[0]
    bands = size // 8
    sub = lax.broadcasted_iota(jnp.int32, (8, 2 * size), 0)
    lane = lax.broadcasted_iota(jnp.int32, (8, 2 * size), 1)
    wide = jnp.concatenate([matrix, jnp.zeros_like(matrix)], axis=1)
    work = [
        jnp.where(lane == size + 8 * b + sub, 1.0, wide[8 * b : 8 * b + 8]) for b in range(bands)
    ]

    def column(value, j):
        place = jnp.full(value.shape, j, jnp.int32)
        return jnp.take_along_axis(value, place, axis=1, mode="promise_in_bounds")

    def line(value, j):
        return jnp.broadcast_to(value[j : j + 1, :], value.shape)

    diagonal = [column(work[0], j) for j in range(8)]
    for b in range(bands):
        cols = {i: [column(work[i], 8 * b + j) for j in range(8)] for i in range(b + 1, bands)}
        coming = [column(work[b + 1], 8 * b + 8 + k) for k in range(8)] if cols else None
        scale = None
        for j in range(8):
            pivot = line(diagonal[j], j)
            root = lax.rsqrt(pivot)
            inverse = root * root
            scale = root if scale is None else jnp.where(sub == j, root, scale)
            lower = jnp.where(sub > j, diagonal[j], 0.0)
            factor = lower * inverse
            ahead = {k: line(diagonal[k], j) for k in range(j + 1, 8)}
            pivot_row = line(work[b], j)
            for k in range(j + 1, 8):
                change = lower * ahead[k] * inverse if k == j + 1 else factor * ahead[k]
                diagonal[k] = diagonal[k] - change
            work[b] = work[b] - factor * pivot_row
            for i in range(b + 1, bands):
                below = cols[i][j] * inverse
                for k in range(j + 1, 8):
                    cols[i][k] = cols[i][k] - below * ahead[k]
                work[i] = work[i] - below * pivot_row
                if i == b + 1:
                    coming = [coming[k] - below * line(cols[i][j], k) for k in range(8)]
        work[b] = work[b] * scale
        diagonal = coming
    return jnp.concatenate(work, axis=0)[:, size:]


def orthonormal(rows):
    split = parts(rows, 3)
    return dot_parts(parts(lower_inverse(dot_parts(split, split, NT)), 3), split, NN)


def upper_pairs(count):
    return [(a, b) for a in range(count) for b in range(a, count)]


def cut(index):
    return slice(index * BLOCK, (index + 1) * BLOCK)


def gram_kernel(core_ref, x_ref, o_ref, held_ref, arrived, *sum_refs):
    steps, deep, width = held_ref.shape
    half = width // 2
    copies = [
        pltpu.make_async_copy(
            x_ref.at[pl.ds(n * deep, deep), :], held_ref.at[n], arrived.at[n]
        )
        for n in range(steps)
    ]
    for copy in copies:
        copy.start()
    left, right = slice(None, half), slice(half, None)
    for n, copy in enumerate(copies):
        copy.wait()
        high, low = parts(held_ref[n], 2)
        high_t = high.T
        found = [
            dot(high_t[left], high[:, left], NN),
            dot(high_t[left], high[:, right], NN),
            dot(high_t[right], high[:, right], NN),
            dot(high_t[left], low[:, left], NN),
            dot(high_t[left], low[:, right], NN),
            dot(high_t[right], low[:, left], NN),
            dot(high_t[right], low[:, right], NN),
        ]
        for ref, value in zip(sum_refs, found):
            ref[...] = value if n == 0 else ref[...] + value
    aa, ab, bb, ll, lr, rl, rr = [ref[...] for ref in sum_refs]
    place = {(0, 0): aa + ll + ll.T, (0, 1): ab + lr + rl.T, (1, 1): bb + rr + rr.T}
    pairs = upper_pairs(width // BLOCK)
    held = len(pairs) // 2
    for n, (a, b) in enumerate(pairs):
        block = place[a // 2, b // 2][cut(a % 2), cut(b % 2)]
        o_ref[(n // held) ^ core_ref[0], cut(n % held), :] = block


def gram(snapshots, core):
    rows, width = snapshots.shape
    steps = 4
    held = len(upper_pairs(width // BLOCK)) // 2 * BLOCK
    return pl.pallas_call(
        gram_kernel,
        in_specs=[SMEM, HBM],
        out_specs=VMEM,
        out_shape=jax.ShapeDtypeStruct((2, held, BLOCK), jnp.float32),
        scratch_shapes=[
            pltpu.VMEM((steps, rows // steps, width), jnp.float32),
            pltpu.SemaphoreType.DMA((steps,)),
        ]
        + [pltpu.VMEM((width // 2, width // 2), jnp.float32)] * 7,
        compiler_params=pltpu.CompilerParams(vmem_limit_bytes=48 * 2**20),
        name="gram",
    )(core, snapshots)


def in_order(core_ref, mine_ref, other_ref):
    first = core_ref[0] == 0
    mine, other = mine_ref[...], other_ref[...]
    return jnp.where(first, mine, other), jnp.where(first, other, mine)


def sweep(rows, gram_refs):
    split = parts(rows, 3)
    ahead = dot_parts(split, [ref[...] for ref in gram_refs], NN)
    return lower_inverse(dot_parts(split, split, NT)), ahead


def normalised(inverse, rows):
    return dot_parts(parts(inverse, 3), parts(rows, 3), NN)


def solve_kernel(row_total, core_ref, mine_ref, other_ref, start_ref, o_ref, next_ref, *gram_refs):
    width = gram_refs[0].shape[0]
    pairs = upper_pairs(width // BLOCK)
    held = len(pairs) // 2
    halves = in_order(core_ref, mine_ref, other_ref)
    for n, (a, b) in enumerate(pairs):
        block = halves[n // held][cut(n % held)] / row_total
        for ref, piece in zip(gram_refs, parts(block, 3)):
            ref[cut(a), cut(b)] = piece
        if a != b:
            for ref, piece in zip(gram_refs, parts(block.T, 3)):
                ref[cut(b), cut(a)] = piece
    next_ref[...] = start_ref[...]

    def step(index, carry):
        next_ref[...] = normalised(*sweep(next_ref[...], gram_refs))
        return carry

    lax.fori_loop(0, ITERS, step, 0)
    o_ref[...] = orthonormal(next_ref[...])


def group_solve(core, mine, other, start, row_total):
    rank, width = start.shape
    return pl.pallas_call(
        lambda *refs: solve_kernel(row_total, *refs),
        in_specs=[SMEM, VMEM, VMEM, VMEM],
        out_specs=VMEM,
        out_shape=jax.ShapeDtypeStruct((rank, width), jnp.float32),
        scratch_shapes=[pltpu.VMEM((rank, width), jnp.float32)]
        + [pltpu.VMEM((width, width), jnp.bfloat16)] * 3,
        compiler_params=pltpu.CompilerParams(vmem_limit_bytes=32 * 2**20),
        name="group_solve",
    )(core, mine, other, start)


def group_basis(basis, snapshots, half):
    rank = basis.shape[0]
    rows = snapshots.shape[0]
    deep = rows // 4

    def kernel(q_ref, x_ref, o_ref, held_ref, arrived):
        copies = [
            pltpu.make_async_copy(
                x_ref.at[pl.ds((half * 2 + n) * deep, deep), :], held_ref.at[n], arrived.at[n]
            )
            for n in range(2)
        ]
        for copy in copies:
            copy.start()
        left = parts(q_ref[...], 2)
        for n, copy in enumerate(copies):
            copy.wait()
            right = parts(held_ref[n], 2)
            o_ref[:, n * deep : (n + 1) * deep] = dot_parts(left, right, NT)

    return pl.pallas_call(
        kernel,
        in_specs=[VMEM, HBM],
        out_specs=VMEM,
        out_shape=jax.ShapeDtypeStruct((rank, rows // 2), jnp.float32),
        scratch_shapes=[
            pltpu.VMEM((2, deep, snapshots.shape[1]), jnp.float32),
            pltpu.SemaphoreType.DMA((2,)),
        ],
        compiler_params=pltpu.CompilerParams(vmem_limit_bytes=48 * 2**20),
        name="group_basis",
    )(basis, snapshots)


def stacked(refs, h):
    return jnp.concatenate([ref[...] for ref in refs[h::2]], axis=0)


def across_products(joined_refs, across_refs, test_ref, h):
    rank, deep = across_refs[0].shape
    cross, last = None, None
    for n in range(2):
        here = slice(n * deep, (n + 1) * deep)
        pieces = [ref[:, here] for ref in joined_refs[h::2]] + [across_refs[2 * h + n][...]]
        left = parts(jnp.concatenate(pieces, axis=0), 2)
        across = [piece[-rank:] for piece in left]
        first = (2 * h + n) * deep
        right = parts(test_ref[first : first + deep, :], 2)
        own = dot_parts(left, across, NT)
        other = dot_parts(across, right, NN)
        cross = own if cross is None else cross + own
        last = other if last is None else last + other
    return cross, last


def merge_near_kernel(test_ref, *refs):
    *all_refs, merged_ref, side_ref, cross_ref, last_ref = refs
    joined_refs, across_refs = all_refs[:-2], all_refs[-2:]
    cross_ref[...], last_ref[...] = across_products(joined_refs, across_refs, test_ref, 0)
    half = joined_refs[0].shape[1]
    merged, side = None, None
    for h in range(2):
        left = parts(stacked(joined_refs, h), 2)
        right = parts(test_ref[h * half : (h + 1) * half, :], 2)
        own = dot_parts(left, left, NT)
        other = dot_parts(left, right, NN)
        merged = own if merged is None else merged + own
        side = other if side is None else side + other
    merged_ref[...] = merged
    side_ref[...] = side


def merge_near(joined, across, test_block):
    rank = joined[0].shape[0]
    wide = len(joined) // 2 * rank
    return pl.pallas_call(
        merge_near_kernel,
        in_specs=[VMEM] * (1 + len(joined) + len(across)),
        out_specs=[VMEM] * 4,
        out_shape=[
            jax.ShapeDtypeStruct((wide, wide), jnp.float32),
            jax.ShapeDtypeStruct((wide, BLOCK), jnp.float32),
            jax.ShapeDtypeStruct((wide + rank, rank), jnp.float32),
            jax.ShapeDtypeStruct((rank, BLOCK), jnp.float32),
        ],
        compiler_params=pltpu.CompilerParams(vmem_limit_bytes=28 * 2**20),
        name="merge_near",
    )(test_block, *joined, *across)


def merge_kernel(place_ref, merged_ref, side_ref, cross_ref, last_ref, test_ref, *refs):
    *all_refs, o_ref = refs
    joined_refs, across_refs = all_refs[:-4], all_refs[-4:]
    rank = across_refs[0].shape[0]
    cross, last = across_products(joined_refs, across_refs, test_ref, 1)
    cross, last = cross + cross_ref[...], last + last_ref[...]
    merged, side = merged_ref[...], side_ref[...]
    blocks = [
        merged[:BLOCK, :BLOCK],
        jnp.concatenate([merged[:BLOCK, BLOCK:], cross[:BLOCK]], axis=1),
        jnp.concatenate(
            [jnp.concatenate([merged[BLOCK:, BLOCK:], cross[BLOCK:-rank].T], axis=0), cross[BLOCK:]],
            axis=1,
        ),
    ]
    side = jnp.concatenate([side, last], axis=0)
    blocks += [side[cut(a), :] for a in range(2)]
    pieces = [block[i * 64 : (i + 1) * 64] for block in blocks for i in range(2)]
    for n, piece in enumerate(pieces):
        o_ref[(n // 5) ^ place_ref[0], (n % 5) * 64 : (n % 5 + 1) * 64, :] = piece


def merge_partials(place, joined, across, test_block):
    return pl.pallas_call(
        merge_kernel,
        in_specs=[SMEM] + [VMEM] * (5 + len(joined) + len(across)),
        out_specs=VMEM,
        out_shape=jax.ShapeDtypeStruct((2, 320, BLOCK), jnp.float32),
        compiler_params=pltpu.CompilerParams(vmem_limit_bytes=28 * 2**20),
        name="merge_partials",
    )(place, *merge_near(joined, across[:2], test_block), test_block, *joined, *across)


def finish_kernel(row_total, place_ref, mine_ref, other_ref, start_ref, *refs):
    *joined_refs, o_ref, next_ref, high_ref, middle_ref, low_ref = refs
    gram_refs = [high_ref, middle_ref, low_ref]
    halves = in_order(place_ref, mine_ref, other_ref)
    pieces = [halves[n // 5][(n % 5) * 64 : (n % 5 + 1) * 64] for n in range(10)]
    blocks = [jnp.concatenate(pieces[2 * n : 2 * n + 2], axis=0) for n in range(5)]
    for (a, b), block in zip(upper_pairs(2), blocks[:3]):
        block = block / row_total
        for ref, piece in zip(gram_refs, parts(block, 3)):
            ref[cut(a), cut(b)] = piece
        if a != b:
            for ref, piece in zip(gram_refs, parts(block.T, 3)):
                ref[cut(b), cut(a)] = piece
    start = start_ref[...]
    rank, wide = start.shape
    groups = len(SHIFTS)
    each = wide // groups
    turned = None
    for g in range(groups):
        firsts = [(g + k) % groups * each for k in SHIFTS]
        order = jnp.concatenate([start[:, f : f + each] for f in firsts], axis=1)
        turned = order if turned is None else jnp.where(place_ref[1] == g, order, turned)
    next_ref[...] = turned

    def step(index, carry):
        next_ref[...] = normalised(*sweep(next_ref[...], gram_refs))
        return carry

    lax.fori_loop(0, ITERS, step, 0)
    inverse, ahead = sweep(next_ref[...], gram_refs)
    coef = parts(normalised(inverse, next_ref[...]), 3)
    energy = dot_parts(parts(normalised(inverse, ahead), 3), coef, NT)
    coef = dot_parts(parts(lower_inverse(energy), 3), coef, NN)
    side = jnp.concatenate(blocks[3:], axis=0)
    test_coeffs = dot_parts(parts(coef, 3), parts(side, 3), NN)
    weight = dot_parts(parts(coef.T, 3), parts(test_coeffs, 3), NN) / row_total
    weight = parts(weight.T, 2)
    across_refs = joined_refs[-4:]
    deep = across_refs[0].shape[1]
    for n in range(4):
        here = slice(n % 2 * deep, (n % 2 + 1) * deep)
        bases = [ref[:, here] for ref in joined_refs[:-4][n // 2 :: 2]] + [across_refs[n][...]]
        joined = jnp.concatenate(bases, axis=0)
        o_ref[n * deep : (n + 1) * deep, :] = dot_parts(weight, parts(joined, 2), NN).T


def finish(place, mine, other, start, joined, across, row_total):
    rank, wide = start.shape
    rows = 2 * joined[0].shape[1]
    return pl.pallas_call(
        lambda *refs: finish_kernel(row_total, *refs),
        in_specs=[SMEM] + [VMEM] * (3 + len(joined) + len(across)),
        out_specs=VMEM,
        out_shape=jax.ShapeDtypeStruct((rows, BLOCK), jnp.float32),
        scratch_shapes=[pltpu.VMEM((rank, wide), jnp.float32)]
        + [pltpu.VMEM((wide, wide), jnp.bfloat16)] * 3,
        compiler_params=pltpu.CompilerParams(vmem_limit_bytes=28 * 2**20),
        name="finish",
    )(place, mine, other, start, *joined, *across)


def swap_cores(array):
    return lax.ppermute(array, CORE, [(0, 1), (1, 0)])


def reduced(array, axis):
    length = lax.axis_size(axis)
    cuts = array.reshape(length, array.shape[0] // length, BLOCK)
    return jnp.sum(lax.all_to_all(cuts, axis, 0, 0, tiled=True), axis=0)


def spread(array, axis):
    copies = jnp.broadcast_to(array, (lax.axis_size(axis), *array.shape))
    return lax.all_to_all(copies, axis, 0, 0, tiled=True)


def sum_over_rows(halves, staged):
    kept = halves[0] + swap_cores(halves[1])
    if staged:
        near, far = CHIPS
        mine = spread(jnp.sum(spread(reduced(kept, near), far), axis=0), near)
    else:
        mine = spread(reduced(kept, CHIPS), CHIPS)
    mine = mine.reshape(kept.shape)
    return mine, swap_cores(mine)


def gathered_bases(near, far):
    groups = lax.axis_size("grp")
    down = [(i, (i - 1) % groups) for i in range(groups)]
    up = [(i, (i + 1) % groups) for i in range(groups)]
    half = near.shape[1] // 2
    next_near = lax.ppermute(near, "grp", down)
    last_near = lax.ppermute(near, "grp", up)
    next_far = lax.ppermute(far, "grp", down)
    last_far = lax.ppermute(far, "grp", up)
    across = [
        lax.ppermute(next_near[:, :half], "grp", down),
        lax.ppermute(last_near[:, half:], "grp", up),
        lax.ppermute(next_far[:, :half], "grp", down),
        lax.ppermute(last_far[:, half:], "grp", up),
    ]
    return [near, far, next_near, next_far, last_near, last_far], across


def on_device(snapshots, test_block, start_block, start_merge):
    row_total = snapshots.shape[0] * lax.axis_size(ROW)
    place = jnp.stack([lax.axis_index(CORE), lax.axis_index("grp")])
    mine, other = sum_over_rows(gram(snapshots, place), False)
    basis = group_solve(place, mine, other, start_block.T, row_total)
    joined, across = gathered_bases(*[group_basis(basis, snapshots, h) for h in range(2)])
    mine, other = sum_over_rows(merge_partials(place, joined, across, test_block), True)
    return finish(place, mine, other, start_merge.T, joined, across, row_total)


def solution(mesh):
    finer = Mesh(
        mesh.devices.reshape(mesh.shape["grp"], 4, 8, 2), ("grp", "row_0", "row_1", "row_2")
    )
    placed = (P(ROW, "grp"), P(ROW, "grp"), P("grp", None), P())
    return jax.shard_map(
        on_device, mesh=finer, in_specs=placed, out_specs=P(ROW, "grp"), check_vma=False
    )
```

```python
import jax
import jax.numpy as jnp
from jax import lax
from jax.experimental import pallas as pl
from jax.experimental.pallas import tpu as pltpu
from jax.sharding import Mesh
from jax.sharding import PartitionSpec as P

ITERS = 6
ROW = ("row_0", "row_1", "row_2")
CHIPS = ("row_0", "row_1")
CORE = "row_2"
BLOCK = 128
SHIFTS = (0, 1, 3, 2)
HBM = pl.BlockSpec(memory_space=pltpu.HBM)
VMEM = pl.BlockSpec(memory_space=pltpu.VMEM)
SMEM = pl.BlockSpec(memory_space=pltpu.SMEM)

NT = (((1,), (1,)), ((), ()))
NN = (((1,), (0,)), ((), ()))
TN = (((0,), (0,)), ((), ()))


def dot(left, right, dims):
    return lax.dot_general(left, right, dims, preferred_element_type=jnp.float32)


def parts(x, count):
    found = []
    for _ in range(count - 1):
        piece = x.astype(jnp.bfloat16)
        found.append(piece)
        x = x - piece.astype(jnp.float32)
    found.append(x.astype(jnp.bfloat16))
    return found


def dot_parts(left, right, dims):
    count = len(left)
    rows = left[0].shape[0]
    total = None
    for j in reversed(range(count)):
        stack = jnp.concatenate(left[: count - j], axis=0) if j < count - 1 else left[0]
        product = dot(stack, right[j], dims)
        for i in reversed(range(count - j)):
            piece = product[i * rows : (i + 1) * rows]
            total = piece if total is None else total + piece
    return total


def lower_inverse(matrix):
    size = matrix.shape[0]
    bands = size // 8
    sub = lax.broadcasted_iota(jnp.int32, (8, 2 * size), 0)
    lane = lax.broadcasted_iota(jnp.int32, (8, 2 * size), 1)
    wide = jnp.concatenate([matrix, jnp.zeros_like(matrix)], axis=1)
    work = [
        jnp.where(lane == size + 8 * b + sub, 1.0, wide[8 * b : 8 * b + 8]) for b in range(bands)
    ]

    def column(value, j):
        place = jnp.full(value.shape, j, jnp.int32)
        return jnp.take_along_axis(value, place, axis=1, mode="promise_in_bounds")

    def line(value, j):
        return jnp.broadcast_to(value[j : j + 1, :], value.shape)

    diagonal = [column(work[0], j) for j in range(8)]
    for b in range(bands):
        cols = {i: [column(work[i], 8 * b + j) for j in range(8)] for i in range(b + 1, bands)}
        coming = [column(work[b + 1], 8 * b + 8 + k) for k in range(8)] if cols else None
        scale = None
        for j in range(8):
            pivot = line(diagonal[j], j)
            root = lax.rsqrt(pivot)
            inverse = root * root
            scale = root if scale is None else jnp.where(sub == j, root, scale)
            lower = jnp.where(sub > j, diagonal[j], 0.0)
            factor = lower * inverse
            ahead = {k: line(diagonal[k], j) for k in range(j + 1, 8)}
            pivot_row = line(work[b], j)
            for k in range(j + 1, 8):
                change = lower * ahead[k] * inverse if k == j + 1 else factor * ahead[k]
                diagonal[k] = diagonal[k] - change
            work[b] = work[b] - factor * pivot_row
            for i in range(b + 1, bands):
                below = cols[i][j] * inverse
                for k in range(j + 1, 8):
                    cols[i][k] = cols[i][k] - below * ahead[k]
                work[i] = work[i] - below * pivot_row
                if i == b + 1:
                    coming = [coming[k] - below * line(cols[i][j], k) for k in range(8)]
        work[b] = work[b] * scale
        diagonal = coming
    return jnp.concatenate(work, axis=0)[:, size:]


def orthonormal(rows):
    split = parts(rows, 3)
    return dot_parts(parts(lower_inverse(dot_parts(split, split, NT)), 3), split, NN)


def upper_pairs(count):
    return [(a, b) for a in range(count) for b in range(a, count)]


def cut(index):
    return slice(index * BLOCK, (index + 1) * BLOCK)


def gram_kernel(core_ref, x_ref, o_ref, held_ref, arrived, *sum_refs):
    steps, deep, width = held_ref.shape
    half = width // 2
    copies = [
        pltpu.make_async_copy(
            x_ref.at[pl.ds(n * deep, deep), :], held_ref.at[n], arrived.at[n]
        )
        for n in range(steps)
    ]
    for copy in copies:
        copy.start()
    left, right = slice(None, half), slice(half, None)
    for n, copy in enumerate(copies):
        copy.wait()
        high, low = parts(held_ref[n], 2)
        high_t = high.T
        found = [
            dot(high_t[left], high[:, left], NN),
            dot(high_t[left], high[:, right], NN),
            dot(high_t[right], high[:, right], NN),
            dot(high_t[left], low[:, left], NN),
            dot(high_t[left], low[:, right], NN),
            dot(high_t[right], low[:, left], NN),
            dot(high_t[right], low[:, right], NN),
        ]
        for ref, value in zip(sum_refs, found):
            ref[...] = value if n == 0 else ref[...] + value
    aa, ab, bb, ll, lr, rl, rr = [ref[...] for ref in sum_refs]
    place = {(0, 0): aa + ll + ll.T, (0, 1): ab + lr + rl.T, (1, 1): bb + rr + rr.T}
    pairs = upper_pairs(width // BLOCK)
    held = len(pairs) // 2
    for n, (a, b) in enumerate(pairs):
        block = place[a // 2, b // 2][cut(a % 2), cut(b % 2)]
        o_ref[(n // held) ^ core_ref[0], cut(n % held), :] = block


def gram(snapshots, core):
    rows, width = snapshots.shape
    steps = 7
    held = len(upper_pairs(width // BLOCK)) // 2 * BLOCK
    return pl.pallas_call(
        gram_kernel,
        in_specs=[SMEM, HBM],
        out_specs=VMEM,
        out_shape=jax.ShapeDtypeStruct((2, held, BLOCK), jnp.float32),
        scratch_shapes=[
            pltpu.VMEM((steps, rows // steps, width), jnp.float32),
            pltpu.SemaphoreType.DMA((steps,)),
        ]
        + [pltpu.VMEM((width // 2, width // 2), jnp.float32)] * 7,
        compiler_params=pltpu.CompilerParams(vmem_limit_bytes=48 * 2**20),
        name="gram",
    )(core, snapshots)


def in_order(core_ref, mine_ref, other_ref):
    first = core_ref[0] == 0
    mine, other = mine_ref[...], other_ref[...]
    return jnp.where(first, mine, other), jnp.where(first, other, mine)


def sweep(rows, gram_refs):
    split = parts(rows, 3)
    ahead = dot_parts(split, [ref[...] for ref in gram_refs], NN)
    return lower_inverse(dot_parts(split, split, NT)), ahead


def normalised(inverse, rows):
    return dot_parts(parts(inverse, 3), parts(rows, 3), NN)


def solve_kernel(row_total, core_ref, mine_ref, other_ref, start_ref, o_ref, next_ref, *gram_refs):
    width = gram_refs[0].shape[0]
    pairs = upper_pairs(width // BLOCK)
    held = len(pairs) // 2
    halves = in_order(core_ref, mine_ref, other_ref)
    for n, (a, b) in enumerate(pairs):
        block = halves[n // held][cut(n % held)] / row_total
        for ref, piece in zip(gram_refs, parts(block, 3)):
            ref[cut(a), cut(b)] = piece
        if a != b:
            for ref, piece in zip(gram_refs, parts(block.T, 3)):
                ref[cut(b), cut(a)] = piece
    next_ref[...] = start_ref[...]

    def step(index, carry):
        next_ref[...] = normalised(*sweep(next_ref[...], gram_refs))
        return carry

    lax.fori_loop(0, ITERS, step, 0)
    o_ref[...] = orthonormal(next_ref[...])


def group_solve(core, mine, other, start, row_total):
    rank, width = start.shape
    return pl.pallas_call(
        lambda *refs: solve_kernel(row_total, *refs),
        in_specs=[SMEM, VMEM, VMEM, VMEM],
        out_specs=VMEM,
        out_shape=jax.ShapeDtypeStruct((rank, width), jnp.float32),
        scratch_shapes=[pltpu.VMEM((rank, width), jnp.float32)]
        + [pltpu.VMEM((width, width), jnp.bfloat16)] * 3,
        compiler_params=pltpu.CompilerParams(vmem_limit_bytes=32 * 2**20),
        name="group_solve",
    )(core, mine, other, start)


def group_basis(basis, snapshots, half):
    rank = basis.shape[0]
    rows = snapshots.shape[0]
    deep = rows // 2
    edges = [0, deep // 7 * 2, deep // 7 * 4, deep]
    spans = list(zip(edges, edges[1:]))

    def kernel(q_ref, x_ref, o_ref, held_ref, arrived):
        copies = [
            pltpu.make_async_copy(
                x_ref.at[pl.ds(half * deep + first, end - first), :],
                held_ref.at[pl.ds(first, end - first), :],
                arrived.at[n],
            )
            for n, (first, end) in enumerate(spans)
        ]
        for copy in copies:
            copy.start()
        left = parts(q_ref[...], 2)
        for copy, (first, end) in zip(copies, spans):
            copy.wait()
            right = parts(held_ref[first:end, :], 2)
            o_ref[:, first:end] = dot_parts(left, right, NT)

    return pl.pallas_call(
        kernel,
        in_specs=[VMEM, HBM],
        out_specs=VMEM,
        out_shape=jax.ShapeDtypeStruct((rank, rows // 2), jnp.float32),
        scratch_shapes=[
            pltpu.VMEM((deep, snapshots.shape[1]), jnp.float32),
            pltpu.SemaphoreType.DMA((len(spans),)),
        ],
        compiler_params=pltpu.CompilerParams(vmem_limit_bytes=48 * 2**20),
        name="group_basis",
    )(basis, snapshots)


def stacked(refs, h):
    return jnp.concatenate([ref[...] for ref in refs[h::2]], axis=0)


def across_products(joined_refs, across_refs, test_ref, h):
    rank, deep = across_refs[0].shape
    across = jnp.concatenate([ref[...] for ref in across_refs[2 * h : 2 * h + 2]], axis=1)
    left = parts(jnp.concatenate([ref[...] for ref in joined_refs[h::2]] + [across], axis=0), 2)
    across = [piece[-rank:] for piece in left]
    right = parts(test_ref[2 * h * deep : 2 * (h + 1) * deep, :], 2)
    return dot_parts(left, across, NT), dot_parts(across, right, NN)


def merge_near_kernel(test_ref, *refs):
    *all_refs, merged_ref, side_ref, cross_ref, last_ref = refs
    joined_refs, across_refs = all_refs[:-2], all_refs[-2:]
    cross_ref[...], last_ref[...] = across_products(joined_refs, across_refs, test_ref, 0)
    half = joined_refs[0].shape[1]
    merged, side = None, None
    for h in range(2):
        left = parts(stacked(joined_refs, h), 2)
        right = parts(test_ref[h * half : (h + 1) * half, :], 2)
        own = dot_parts(left, left, NT)
        other = dot_parts(left, right, NN)
        merged = own if merged is None else merged + own
        side = other if side is None else side + other
    merged_ref[...] = merged
    side_ref[...] = side


def merge_near(joined, across, test_block):
    rank = joined[0].shape[0]
    wide = len(joined) // 2 * rank
    return pl.pallas_call(
        merge_near_kernel,
        in_specs=[VMEM] * (1 + len(joined) + len(across)),
        out_specs=[VMEM] * 4,
        out_shape=[
            jax.ShapeDtypeStruct((wide, wide), jnp.float32),
            jax.ShapeDtypeStruct((wide, BLOCK), jnp.float32),
            jax.ShapeDtypeStruct((wide + rank, rank), jnp.float32),
            jax.ShapeDtypeStruct((rank, BLOCK), jnp.float32),
        ],
        compiler_params=pltpu.CompilerParams(vmem_limit_bytes=28 * 2**20),
        name="merge_near",
    )(test_block, *joined, *across)


def merge_kernel(place_ref, merged_ref, side_ref, cross_ref, last_ref, test_ref, *refs):
    *all_refs, o_ref = refs
    joined_refs, across_refs = all_refs[:-4], all_refs[-4:]
    rank = across_refs[0].shape[0]
    cross, last = across_products(joined_refs, across_refs, test_ref, 1)
    cross, last = cross + cross_ref[...], last + last_ref[...]
    merged, side = merged_ref[...], side_ref[...]
    blocks = [
        merged[:BLOCK, :BLOCK],
        jnp.concatenate([merged[:BLOCK, BLOCK:], cross[:BLOCK]], axis=1),
        jnp.concatenate(
            [jnp.concatenate([merged[BLOCK:, BLOCK:], cross[BLOCK:-rank].T], axis=0), cross[BLOCK:]],
            axis=1,
        ),
    ]
    side = jnp.concatenate([side, last], axis=0)
    blocks += [side[cut(a), :] for a in range(2)]
    pieces = [block[i * 64 : (i + 1) * 64] for block in blocks for i in range(2)]
    for n, piece in enumerate(pieces):
        o_ref[(n // 5) ^ place_ref[0], (n % 5) * 64 : (n % 5 + 1) * 64, :] = piece


def merge_partials(place, joined, across, test_block):
    return pl.pallas_call(
        merge_kernel,
        in_specs=[SMEM] + [VMEM] * (5 + len(joined) + len(across)),
        out_specs=VMEM,
        out_shape=jax.ShapeDtypeStruct((2, 320, BLOCK), jnp.float32),
        compiler_params=pltpu.CompilerParams(vmem_limit_bytes=28 * 2**20),
        name="merge_partials",
    )(place, *merge_near(joined, across[:2], test_block), test_block, *joined, *across)


def finish_kernel(row_total, place_ref, mine_ref, other_ref, start_ref, *refs):
    *joined_refs, o_ref, next_ref, high_ref, middle_ref, low_ref = refs
    gram_refs = [high_ref, middle_ref, low_ref]
    halves = in_order(place_ref, mine_ref, other_ref)
    pieces = [halves[n // 5][(n % 5) * 64 : (n % 5 + 1) * 64] for n in range(10)]
    blocks = [jnp.concatenate(pieces[2 * n : 2 * n + 2], axis=0) for n in range(5)]
    for (a, b), block in zip(upper_pairs(2), blocks[:3]):
        block = block / row_total
        for ref, piece in zip(gram_refs, parts(block, 3)):
            ref[cut(a), cut(b)] = piece
        if a != b:
            for ref, piece in zip(gram_refs, parts(block.T, 3)):
                ref[cut(b), cut(a)] = piece
    start = start_ref[...]
    rank, wide = start.shape
    groups = len(SHIFTS)
    each = wide // groups
    turned = None
    for g in range(groups):
        firsts = [(g + k) % groups * each for k in SHIFTS]
        order = jnp.concatenate([start[:, f : f + each] for f in firsts], axis=1)
        turned = order if turned is None else jnp.where(place_ref[1] == g, order, turned)
    next_ref[...] = turned

    def step(index, carry):
        next_ref[...] = normalised(*sweep(next_ref[...], gram_refs))
        return carry

    lax.fori_loop(0, ITERS, step, 0)
    inverse, ahead = sweep(next_ref[...], gram_refs)
    coef = parts(normalised(inverse, next_ref[...]), 3)
    energy = dot_parts(parts(normalised(inverse, ahead), 3), coef, NT)
    coef = dot_parts(parts(lower_inverse(energy), 3), coef, NN)
    side = jnp.concatenate(blocks[3:], axis=0)
    test_coeffs = dot_parts(parts(coef, 3), parts(side, 3), NN)
    weight = dot_parts(parts(coef.T, 3), parts(test_coeffs, 3), NN) / row_total
    weight = parts(weight.T, 2)
    across_refs = joined_refs[-4:]
    half = joined_refs[0].shape[1]
    for h in range(2):
        across = jnp.concatenate([ref[...] for ref in across_refs[2 * h : 2 * h + 2]], axis=1)
        bases = [ref[...] for ref in joined_refs[:-4][h::2]] + [across]
        joined = parts(jnp.concatenate(bases, axis=0), 2)
        o_ref[h * half : (h + 1) * half, :] = dot_parts(weight, joined, NN).T


def finish(place, mine, other, start, joined, across, row_total):
    rank, wide = start.shape
    rows = 2 * joined[0].shape[1]
    return pl.pallas_call(
        lambda *refs: finish_kernel(row_total, *refs),
        in_specs=[SMEM] + [VMEM] * (3 + len(joined) + len(across)),
        out_specs=VMEM,
        out_shape=jax.ShapeDtypeStruct((rows, BLOCK), jnp.float32),
        scratch_shapes=[pltpu.VMEM((rank, wide), jnp.float32)]
        + [pltpu.VMEM((wide, wide), jnp.bfloat16)] * 3,
        compiler_params=pltpu.CompilerParams(vmem_limit_bytes=28 * 2**20),
        name="finish",
    )(place, mine, other, start, *joined, *across)


def swap_cores(array):
    return lax.ppermute(array, CORE, [(0, 1), (1, 0)])


def reduced(array, axis):
    length = lax.axis_size(axis)
    cuts = array.reshape(length, array.shape[0] // length, BLOCK)
    return jnp.sum(lax.all_to_all(cuts, axis, 0, 0, tiled=True), axis=0)


def spread(array, axis):
    copies = jnp.broadcast_to(array, (lax.axis_size(axis), *array.shape))
    return lax.all_to_all(copies, axis, 0, 0, tiled=True)


def sum_over_rows(halves, staged):
    kept = halves[0] + swap_cores(halves[1])
    if staged:
        near, far = CHIPS
        mine = spread(jnp.sum(spread(reduced(kept, near), far), axis=0), near)
    else:
        mine = spread(reduced(kept, CHIPS), CHIPS)
    mine = mine.reshape(kept.shape)
    return mine, swap_cores(mine)


def gathered_bases(near, far):
    groups = lax.axis_size("grp")
    down = [(i, (i - 1) % groups) for i in range(groups)]
    up = [(i, (i + 1) % groups) for i in range(groups)]
    half = near.shape[1] // 2
    next_near = lax.ppermute(near, "grp", down)
    last_near = lax.ppermute(near, "grp", up)
    next_far = lax.ppermute(far, "grp", down)
    last_far = lax.ppermute(far, "grp", up)
    across = [
        lax.ppermute(next_near[:, :half], "grp", down),
        lax.ppermute(last_near[:, half:], "grp", up),
        lax.ppermute(next_far[:, :half], "grp", down),
        lax.ppermute(last_far[:, half:], "grp", up),
    ]
    return [near, far, next_near, next_far, last_near, last_far], across


def on_device(snapshots, test_block, start_block, start_merge):
    row_total = snapshots.shape[0] * lax.axis_size(ROW)
    place = jnp.stack([lax.axis_index(CORE), lax.axis_index("grp")])
    mine, other = sum_over_rows(gram(snapshots, place), False)
    basis = group_solve(place, mine, other, start_block.T, row_total)
    joined, across = gathered_bases(*[group_basis(basis, snapshots, h) for h in range(2)])
    mine, other = sum_over_rows(merge_partials(place, joined, across, test_block), True)
    return finish(place, mine, other, start_merge.T, joined, across, row_total)


def solution(mesh):
    finer = Mesh(
        mesh.devices.reshape(mesh.shape["grp"], 4, 8, 2), ("grp", "row_0", "row_1", "row_2")
    )
    placed = (P(ROW, "grp"), P(ROW, "grp"), P("grp", None), P())
    return jax.shard_map(
        on_device, mesh=finer, in_specs=placed, out_specs=P(ROW, "grp"), check_vma=False
    )
```
